512 devices in a mesh: groups: 2 (over y), word: 32 (over z), sub: 8 (over x, core).
Axes of the slice: x: 4, y: 2, z: 32, core: 2. Of those that a mesh axis runs over, the one named last changes fastest.
The devices are a block of a 4x16x32 slice.
Arguments:
- word_ids: int32 [32, 32, 4096], P('word', None, 'groups'), parts along dimension 2, may hold values from 0 to 32767
- word_weights: float32 [32, 32, 4096], P('word', None, 'groups'), parts along dimension 2, may hold values from 0.25 to 12
- neighbours: int32 [50, 4096], P(None, 'groups'), parts along dimension 1, may hold values from 0 to 2047
- descriptors: bfloat16 [4096, 128, 128], P(('groups', 'word'), 'sub'), parts along dimension 0, may hold values from -6 to 6
- keypoint_count: int32 [4096], P('groups'), parts along dimension 0, may hold values from 32 to 128
- send_table: int32 [64, 32, 8, 2], P('groups'), parts along dimension 0, may hold values from 0 to 63
- pair_slots: int32 [64, 8, 32, 2], P(('groups', 'word'), 'sub'), parts along dimension 0, may hold values from 0 to 63, as said below
Outputs:
- similarity: float32 [4096, 50], P(('groups', 'word', 'sub')), parts along dimension 0
- nearest: float32 [64, 8, 32, 128], P(('groups', 'word'), 'sub'), parts along dimension 0
- margin: float32 [64, 8, 32, 128], P(('groups', 'word'), 'sub'), parts along dimension 0
The draws below stay inside these ranges and needn't reach their ends.
There are 2 independent parts, one for each index of `groups`. The reference program is written for one: setup_inputs(seed, part) draws one part's arguments, and reference() takes and returns one part's arrays. A program takes and returns all parts, laid end to end along the dimension named above; each array names one. Nothing has to cross between parts.
Inputs may be any that keep to these rules, and one draw needn't show every extreme that they name: `word_ids`: each image has 32 word occurrences in every vocabulary shard, given as word numbers within that shard; a number may repeat. `keypoint_count`: keypoint slots at and beyond an image's count are padding. send_table[v, w, s, c] is an image counted among word index v's 64 stored images; every device receives exactly 2 images from every word index, and one image may go to many devices. `pair_slots`: the two slots of a pair are different slots among the 64 of that device, the query first.
All inputs are finite; a program needn't handle non-finite values.
Results may differ from the reference program's by a relative error of at most 0.0003.
Values may be sent and summed in bfloat16 or wider, within the bound.
No kernel may reach another device: no remote copies, remote signals or barrier semaphores. Data moves between devices by JAX's collectives and lax.ppermute only.
A program may use at most 64 MiB of HBM per device.

```python
import math
import jax
import jax.numpy as jnp
import numpy as np
from jax import lax

DESC = 128
VOCAB_DEV = 32768
TOPK = 50
CAP = 2
KP = 128
IMG_DEV = 64
SLOTS = 32
PAIR_DEV = 32
SHARDS = 32
SUBS = 8
IMAGES = 2048
HELD = 64


def draw_word_weights(key, part):
    array_shape = (SHARDS, SLOTS, IMAGES)
    shard_ramp = 1.0 + 2.0 * jnp.arange(SHARDS, dtype=jnp.float32) / max(SHARDS - 1, 1)
    factor = jnp.exp(jax.random.uniform(key, array_shape, jnp.float32, math.log(0.25), math.log(4.0)))
    return (factor * shard_ramp[:, None, None]).astype(jnp.float32)


def draw_pair_slots(key, part):
    first_key, second_key = jax.random.split(key)
    query_slot = jax.random.randint(first_key, (SHARDS, SUBS, PAIR_DEV, 1), 0, HELD)
    offset = jax.random.randint(second_key, (SHARDS, SUBS, PAIR_DEV, 1), 1, HELD)
    return jnp.concatenate([query_slot, (query_slot + offset) % HELD], axis=3).astype(jnp.int32)


def plant(array, key, low, high):
    longest = array.shape.index(max(array.shape))
    spots = []
    for shift in (0, 1):
        where = [jax.random.randint(jax.random.fold_in(key, axis), (), 0, length) for axis, length in enumerate(array.shape)]
        where[longest] = (where[longest] + shift) % array.shape[longest]
        spots.append(tuple(where))
    return array.at[spots[0]].set(low).at[spots[1]].set(high)


def block_scale(rng, shape, shards, low, largest):
    gain, own = 1.0, jax.random.fold_in(rng, 6)
    for dim, blocks in shards:
        heights = jnp.exp(jax.random.uniform(jax.random.fold_in(own, dim), (blocks,), jnp.float32, low / len(shards), largest / len(shards)))
        gain = gain * jnp.repeat(heights, shape[dim] // blocks).reshape([-1 if axis == dim else 1 for axis in range(len(shape))])
    return gain


def rank_table(count, lean):
    weights = [(1 << 20) // math.isqrt(rank ** lean) + 1 for rank in range(1, count + 1)]
    spread = 1 + sum(weights) // (1 << 30)
    return np.cumsum(np.array([max(1, weight // spread) for weight in weights]))


def skewed_ids(stream_key, dims, amount, lean):
    grid = rank_table(amount, lean)
    ticket = jax.random.randint(jax.random.fold_in(stream_key, 1), dims, 0, int(grid[amount - 1]))
    standing = jnp.searchsorted(jnp.asarray(grid, jnp.int32), ticket, side="right")
    return jax.random.permutation(jax.random.fold_in(stream_key, 2), amount)[standing].astype(jnp.int32)


def noise(stream_key, extent, scale, most, cuts=(), kind=jnp.bfloat16):
    drawn = jax.random.normal(stream_key, extent, jnp.float32) * scale
    if len(cuts) > 0:
        drawn = block_scale(stream_key, extent, cuts, -0.22, 0.18) * drawn
    return jnp.clip(drawn, min=-most, max=most).astype(kind)


def setup_inputs(seed: int = 0, part: int = 0) -> dict:
    key_of = jax.random.split(jax.random.key(seed), 8)
    own_keys = jax.random.split(jax.random.fold_in(key_of[7], part), 8)
    word_ids = plant(skewed_ids(own_keys[0], (SHARDS, SLOTS, IMAGES), VOCAB_DEV, 2), jax.random.fold_in(own_keys[0], 3), 0, VOCAB_DEV - 1).astype(jnp.int32)
    word_weights = draw_word_weights(jax.random.fold_in(jax.random.fold_in(key_of[7], part), 71), part)
    neighbours = plant(jax.random.randint(own_keys[2], (TOPK, IMAGES), 0, IMAGES), jax.random.fold_in(own_keys[2], 1), 0, IMAGES - 1).astype(jnp.int32)
    descriptors = noise(own_keys[3], (IMAGES, DESC, KP), 1.0, 6.0, ((0, 32), (1, 8)))
    keypoint_count = plant(jax.random.randint(own_keys[4], (IMAGES,), KP // 4, KP + 1), jax.random.fold_in(own_keys[4], 1), KP // 4, KP).astype(jnp.int32)
    send_table = plant(jax.random.randint(own_keys[5], (SHARDS, SHARDS, SUBS, CAP), 0, IMG_DEV), jax.random.fold_in(own_keys[5], 1), 0, IMG_DEV - 1).astype(jnp.int32)
    pair_slots = draw_pair_slots(jax.random.fold_in(jax.random.fold_in(key_of[7], part), 71), part)
    return dict(word_ids=word_ids, word_weights=word_weights, neighbours=neighbours, descriptors=descriptors, keypoint_count=keypoint_count, send_table=send_table, pair_slots=pair_slots)


def pair_products(row_ids, row_values, other_ids, other_values):
    matches = row_ids[:, :, :, None] == other_ids[:, :, None, :]
    weights = row_values[:, :, :, None] * other_values[:, :, None, :]
    return lax.optimization_barrier(jnp.sum(jnp.where(matches, weights, jnp.float32(0.0)), axis=(2, 3)))

def blocked(function, arrays, block_width):
    row_total = arrays[0].shape[0]
    block_rows = math.gcd(row_total, block_width)
    shaped = tuple((member.reshape((row_total // block_rows, block_rows) + member.shape[1:]) for member in arrays))
    result = lax.map(lambda bundle: function(*bundle), shaped)
    return jax.tree.map(lambda output: output.reshape((row_total,) + output.shape[2:]), result)

def finish(squared, query_count, refer_count, feature_width):
    positions = jnp.arange(squared.shape[-1], dtype=jnp.int32)
    masked = jnp.where(positions[None, None, :] < refer_count[:, None, None], squared, jnp.inf)
    best_value = lax.optimization_barrier(jnp.min(masked, axis=-1))
    at_best = masked == best_value[..., None]
    ties = lax.optimization_barrier(jnp.sum(at_best.astype(jnp.int32), axis=-1))
    others = lax.optimization_barrier(jnp.min(jnp.where(at_best, jnp.inf, masked), axis=-1))
    second = jnp.where(ties > 1, best_value, others)
    live_rows = positions[None, :] < query_count[:, None]
    nearest = jnp.where(live_rows, best_value / feature_width, jnp.float32(0.0))
    margin = jnp.where(live_rows, (second - best_value) / feature_width, jnp.float32(0.0))
    return (nearest, margin)

def shard_terms(shard_ids, shard_values, neighbours):

    def self_block(row_ids, row_values):
        return pair_products(row_ids[:, None, :], row_values[:, None, :], row_ids[:, None, :], row_values[:, None, :])[:, 0]

    def neighbour_block(row_ids, row_values, row_neighbours):
        return pair_products(row_ids[:, None, :], row_values[:, None, :], shard_ids[row_neighbours], shard_values[row_neighbours])
    self_terms = blocked(self_block, (shard_ids, shard_values), 256)
    cross_terms = blocked(neighbour_block, (shard_ids, shard_values, neighbours), 16)
    return (self_terms, cross_terms)

def reference(word_ids, word_weights, neighbours, descriptors, keypoint_count, send_table, pair_slots):
    word_rows = jnp.transpose(word_ids, (0, 2, 1))
    weight_rows = jnp.transpose(word_weights, (0, 2, 1))
    neighbour_rows = jnp.transpose(neighbours, (1, 0))
    self_terms, cross_terms = lax.map(lambda bundle: shard_terms(bundle[0], bundle[1], neighbour_rows), (word_rows, weight_rows))
    norm_sq = lax.optimization_barrier(jnp.sum(self_terms, axis=0))
    dot_sums = lax.optimization_barrier(jnp.sum(cross_terms, axis=0))
    similarity = dot_sums / jnp.sqrt(norm_sq[:, None] * norm_sq[neighbour_rows])
    source_base = (jnp.arange(SHARDS, dtype=jnp.int32) * IMG_DEV)[:, None, None, None]
    slot_image = jnp.transpose(send_table + source_base, (1, 2, 0, 3)).reshape(SHARDS, SUBS, HELD)
    query_image = jnp.take_along_axis(slot_image, pair_slots[:, :, :, 0], axis=2).reshape(-1)
    refer_image = jnp.take_along_axis(slot_image, pair_slots[:, :, :, 1], axis=2).reshape(-1)
    squared_norm = blocked(lambda member: lax.optimization_barrier(jnp.sum(jnp.square(member.astype(jnp.float32)), axis=1)), (descriptors,), 64)

    def match_block(query_rows, refer_rows):
        query_desc = descriptors[query_rows].astype(jnp.float32)
        refer_desc = descriptors[refer_rows].astype(jnp.float32)
        inner_prod = jnp.einsum('bfm,bfn->bmn', query_desc, refer_desc, precision=lax.Precision.HIGHEST)
        squared = squared_norm[query_rows][:, :, None] + squared_norm[refer_rows][:, None, :] - 2.0 * inner_prod
        return finish(squared, keypoint_count[query_rows], keypoint_count[refer_rows], DESC)
    nearest, margin = blocked(match_block, (query_image, refer_image), 4)
    nearest = nearest.reshape(SHARDS, SUBS, PAIR_DEV, KP)
    margin = margin.reshape(SHARDS, SUBS, PAIR_DEV, KP)
    return (similarity, nearest, margin)
```

```python
import functools

import jax
import jax.numpy as jnp
from jax import lax
from jax.experimental import pallas as pl
from jax.experimental.pallas import tpu as pltpu
from jax.sharding import PartitionSpec as P

INTERPRET = False
F32, BF16, I32 = jnp.float32, jnp.bfloat16, jnp.int32
LANES = 128
PENALTY = 1e30
SMEM = pltpu.SMEM
VMEM = pltpu.VMEM
GROUPS = (8, 12, 16)


def call(body, outs, ins, specs=None, scratch=(), mebibytes=2):
    specs = specs or [vm() for _ in ins]
    single = not isinstance(outs, (list, tuple))
    out_list = [outs] if single else list(outs)
    ins = [
        pltpu.with_memory_space_constraint(x, VMEM) if spec.memory_space is VMEM and not INTERPRET else x
        for x, spec in zip(ins, specs)
    ]
    gridded = any(spec.block_shape is not None for spec in specs)
    result = pl.pallas_call(
        body,
        out_shape=[x if INTERPRET else VMEM(x.shape, x.dtype) for x in out_list],
        in_specs=specs,
        out_specs=[vm() for _ in out_list],
        **({"grid": (1,)} if gridded else {}),
        scratch_shapes=list(scratch),
        compiler_params=pltpu.CompilerParams(vmem_limit_bytes=mebibytes << 20),
        interpret=INTERPRET,
    )(*ins)
    return result[0] if single else result


def vm():
    return pl.BlockSpec(memory_space=VMEM)


def sm():
    return pl.BlockSpec(memory_space=SMEM)


def struct(shape, dtype=BF16):
    return jax.ShapeDtypeStruct(shape, dtype)


def rounded(x):
    return x.astype(BF16).astype(F32)


def split3(x):
    first = rounded(x)
    rest = x - first
    second = rounded(rest)
    return first, second, rounded(rest - second)


def encode(norms, dots):
    high = rounded(norms)
    low = rounded(norms - high)
    return jnp.concatenate((high, low) + split3(dots), axis=0).astype(BF16)


def decode(tile):
    wide = tile.astype(F32)
    norms = wide[0:2] + wide[2:4]
    dots = (wide[4:8] + wide[8:12]) + wide[12:16]
    return norms, dots, wide[0:4]


def re_encode(head, dots):
    return jnp.concatenate((head,) + split3(dots), axis=0).astype(BF16)


def spread(rows):
    turned = pltpu.roll(rows, 64, 1)
    low = lax.broadcasted_iota(I32, rows.shape, 1) < 64
    return jnp.where(low, rows, turned), jnp.where(low, turned, rows)


def staggered(four):
    group = lax.broadcasted_iota(I32, four.shape, 1) // 32
    out = four
    for g in range(1, 4):
        out = jnp.where(group == g, pltpu.roll(four, LANES - 8 * g, 1), out)
    return out


def lane_sums(products):
    ones = jnp.ones((8, LANES), F32)
    return lax.dot_general(
        ones, products, (((1,), (1,)), ((), ())), precision=lax.Precision.HIGHEST, preferred_element_type=F32
    )


def norm_kernel(rows_ref, out_ref):
    def step(i, carry):
        start = pl.multiple_of(i * 8, 8)
        ids, weights = spread(rows_ref[pl.ds(start, 8), :])
        other, value = staggered(ids), staggered(weights)
        acc = jnp.zeros_like(ids)
        for t in range(8):
            moved = pltpu.roll(other, LANES - t, 1) if t else other
            scale = pltpu.roll(value, LANES - t, 1) if t else value
            acc = acc + jnp.where(ids == moved, scale, 0.0)
        carry[pl.ds(start, 8), :] = acc * weights
        return None

    def whole(products):
        lax.fori_loop(0, rows_ref.shape[0] // 8, lambda i, c: step(i, products) or c, 0)
        sums = lane_sums(products[...])
        for j in range(rows_ref.shape[0] // LANES):
            out_ref[j : j + 1, :] = sums[0:1, j * LANES : (j + 1) * LANES]

    pl.run_scoped(whole, pltpu.VMEM(rows_ref.shape, F32))


def cross_kernel(count, table_ref, rows_f, rows_b, idx_f, idx_b, dep_ref, out_ref, turned, gathered, products):
    del dep_ref
    padded = gathered.shape[0]
    images = rows_f.shape[1]
    gathered[...] = jnp.zeros_like(gathered)
    products[...] = jnp.zeros_like(products)
    for which, (rows_ref, idx_ref) in enumerate(((rows_f, idx_f), (rows_b, idx_b))):
        ids, weights = spread(rows_ref[0])
        other, value = staggered(ids), staggered(weights)
        for t in range(8):
            turned[0, t] = pltpu.roll(other, LANES - t, 1) if t else other
            turned[1, t] = pltpu.roll(value, LANES - t, 1) if t else value

        def image(i, carry):
            for k in range(count):
                row = idx_ref[0, 0, i * count + k]
                gathered[k : k + 1, :] = table_ref[row]
            queries = [turned[0, t, pl.ds(i, 1), :] for t in range(8)]
            scales = [turned[1, t, pl.ds(i, 1), :] for t in range(8)]
            for part in range(padded // 8):
                near_ids, near_weights = spread(gathered[part * 8 : part * 8 + 8, :])
                acc = jnp.zeros_like(near_ids)
                for t in range(8):
                    acc = acc + jnp.where(near_ids == queries[t], scales[t], 0.0)
                start = pl.multiple_of(i * padded + part * 8, 8)
                products[pl.ds(start, 8), :] = acc * near_weights
            return carry

        lax.fori_loop(0, images, image, 0)
        sums = lane_sums(products[...])
        for j in range(4):
            out_ref[which, j : j + 1, :] = sums[0:1, j * LANES : (j + 1) * LANES]


def first_kernel(desc_ref, norm_ref, cross_ref, out_f, out_b):
    half = desc_ref.shape[0] // 2
    for out, which in ((out_f, 0), (out_b, 1)):
        out[0:half] = desc_ref[half:]
        out[half] = encode(norm_ref[...], cross_ref[which])


def merge_kernel(recv_f, recv_b, norm_ref, cross_ref, out_f, out_b, norm_out):
    half = recv_f.shape[0] - 1
    total = norm_ref[...]
    for recv, out, which in ((recv_f, out_f, 0), (recv_b, out_b, 1)):
        norms, dots, head = decode(recv[half])
        out[0:half] = recv[0:half]
        out[half] = re_encode(head, dots + cross_ref[which])
        total = total + norms
    norm_out[...] = total


def pick(first, second, index):
    half = first.shape[0]
    near = jnp.minimum(index, half - 1)
    far = jnp.maximum(index - half, 0)
    return jnp.where(index < half, first[near].astype(F32), second[far].astype(F32)).astype(BF16)


def trim_kernel(targets, idx, a_f, b_f, a_b, b_b, norm_ref, cross_ref, oa_f, ob_f, oa_b, ob_b, norm_out):
    half = a_f.shape[0]
    total = norm_ref[...]
    for which, (a, b, oa, ob) in enumerate(((a_f, b_f, oa_f, ob_f), (a_b, b_b, oa_b, ob_b))):
        base = which * 4 * targets
        for n in range(targets):
            oa[n] = pick(a, b, idx[base + n])
            ob[n] = pick(a, b, idx[base + targets + n])
            ob[targets + n] = pick(a, b, idx[base + 2 * targets + n])
        for n in range(targets // 2):
            oa[targets + n] = pick(a, b, idx[base + 3 * targets + which * (targets // 2) + n])
        norms, dots, head = decode(b[half])
        ob[2 * targets] = re_encode(head, dots + cross_ref[which])
        total = total + norms
    norm_out[...] = total


def after_trim_kernel(targets, a_f, b_f, a_b, b_b, norm_ref, cross_ref, oa_f, ob_f, oa_b, ob_b, norm_out):
    total = norm_ref[...]
    for which, (a, b, oa, ob) in enumerate(((a_f, b_f, oa_f, ob_f), (a_b, b_b, oa_b, ob_b))):
        norms, dots, head = decode(b[2 * targets])
        oa[0:targets] = b[0:targets]
        oa[targets] = re_encode(head, dots + cross_ref[which])
        ob[0:targets] = b[targets : 2 * targets]
        ob[targets:] = a[targets:]
        total = total + norms
    norm_out[...] = total


def join_kernel(targets, a_f, b_f, a_b, b_b, norm_ref, cross_ref, o_f, o_b, norm_out):
    total = norm_ref[...]
    size = b_f.shape[0]
    for which, (a, b, o) in enumerate(((a_f, b_f, o_f), (a_b, b_b, o_b))):
        norms, dots, head = decode(a[targets])
        o[0:size] = b[...]
        o[size] = re_encode(head, dots + cross_ref[which])
        total = total + norms
    norm_out[...] = total


def last_kernel(targets, c_f, c_b, norm_ref, cross_ref, o_f, o_b, norm_out, dots_out):
    size = targets // 2
    norms_f, dots_f, head = decode(c_f[targets + size])
    o_f[0:size] = c_f[targets : targets + size]
    o_f[size] = re_encode(head, dots_f + cross_ref[0])
    norms_b, dots_b, _ = decode(c_b[targets + size])
    o_b[...] = c_b[targets : targets + size]
    norm_out[...] = norm_ref[...] + norms_f + norms_b
    dots_out[...] = dots_b + cross_ref[1]


def select_kernel(subs, offset, kinds, idx, *refs):
    out = refs[-1]
    position = 0
    for j, kind in enumerate(kinds):
        for s in range(subs):
            for c in range(2):
                slot = idx[(offset + j) * 2 * subs + s * 2 + c]
                if kind == 1:
                    out[s, 2 * j + c] = refs[position][slot]
                else:
                    out[s, 2 * j + c] = pick(refs[position], refs[position + 1], slot)
        position += kind


def tail_kernel(targets, a13f, a13b, a14f, a14b, c15f, c15b, c16f, c16b, norm_ref, dots_ref, out, dots_out):
    subs = targets // 2
    size = targets // 2
    for j, src in enumerate((a13f, a13b, a14f, a14b, c15f, c15b)):
        for s in range(subs):
            out[s, 2 * j : 2 * j + 2] = src[2 * s : 2 * s + 2]
    for s in range(subs):
        src = c16f if s < subs // 2 else c16b
        at = 2 * (s % (subs // 2))
        out[s, 12:14] = src[at : at + 2]
    norms, dots, _ = decode(c16f[size])
    total = norm_ref[...] + norms
    dots_out[...] = dots_ref[...] + dots
    tile = jnp.concatenate(split3(total) + (jnp.zeros((10, LANES), F32),), axis=0).astype(BF16)
    for s in range(subs):
        out[s, 14] = tile


def match_kernel(counts, width, topk, padded, pairs, *refs):
    groups = refs[: len(counts)]
    (pen, live, dots, near_row, near_lane, own_row, own_lane) = refs[len(counts) : len(counts) + 7]
    nearest, margin, similarity = refs[len(counts) + 7 : len(counts) + 10]
    lhs, rhs, squares, least, less, query = refs[len(counts) + 10 :]
    pair_total = nearest.shape[0]
    subs = groups[0].shape[0]
    depth = groups[0].shape[2]
    wide = subs * depth

    rows = []
    for s in range(subs):
        tile = groups[-1][s, counts[-1]].astype(F32)
        rows.append((tile[0:2] + tile[2:4]) + tile[4:6])
    shape = near_row.shape
    near = jnp.zeros(shape, F32)
    own = jnp.zeros(shape, F32)
    for s in range(subs):
        for h in range(2):
            line = jnp.broadcast_to(rows[s][h : h + 1], shape)
            at = jnp.take_along_axis(line, near_lane[...], axis=1)
            near = jnp.where(near_row[...] == 2 * s + h, at, near)
            at = jnp.take_along_axis(line, own_lane[...], axis=1)
            own = jnp.where(own_row[...] == 2 * s + h, at, own)
    cosine = dots[...] / jnp.sqrt(own * near)
    for r in range(similarity.shape[0]):
        line, lane = divmod(r * padded, LANES)
        both = jnp.concatenate((cosine[line : line + 1], cosine[line + 1 : line + 2]), axis=1) if line < 3 else cosine[3:4]
        similarity[r : r + 1, :] = both[:, lane : lane + topk]

    base = 0
    tail = rhs.shape[1] - wide
    row = lax.broadcasted_iota(I32, (tail, LANES), 0)
    ones = jnp.where(row < 4, 1.0, 0.0).astype(BF16)
    for group, count in zip(groups, counts):

        def image(j, carry, group=group, base=base):
            slot = base + j
            total = jnp.zeros((depth, LANES), F32)
            for s in range(subs):
                block = group[s, j]
                rhs[slot, s * depth : (s + 1) * depth, :] = block
                value = block.astype(F32)
                lhs[slot, s * depth : (s + 1) * depth, :] = (value * -2.0).astype(BF16)
                total = total + value * value
            square = jnp.sum(total, axis=0, keepdims=True)
            squares[pl.ds(slot, 1), :] = square
            parts = split3(square)
            extra = jnp.where(row == 0, parts[0], 0.0)
            extra = jnp.where(row == 1, parts[1], extra)
            extra = jnp.where(row == 2, parts[2], extra)
            extra = jnp.where(row == 3, pen[pl.ds(slot, 1), :], extra)
            lhs[slot, wide:, :] = extra.astype(BF16)
            rhs[slot, wide:, :] = ones
            return carry

        lax.fori_loop(0, count, image, 0)
        base += count

    def pair(p, carry):
        asked = pairs[2 * p]
        refer = pairs[2 * p + 1]
        scores = lax.dot_general(
            lhs[refer], rhs[asked], (((0,), (0,)), ((), ())), preferred_element_type=F32
        )
        first = scores[0:8]
        second = jnp.full_like(first, PENALTY)
        for b in range(1, LANES // 8):
            value = scores[8 * b : 8 * b + 8]
            second = jnp.minimum(second, jnp.maximum(first, value))
            first = jnp.minimum(first, value)
        least[p] = first
        less[p] = second
        query[pl.ds(p, 1), :] = squares[pl.ds(asked, 1), :]
        return carry

    lax.fori_loop(0, pair_total, pair, 0)
    first = least[:, 0, :]
    second = less[:, 0, :]
    for b in range(1, 8):
        other, runner = least[:, b, :], less[:, b, :]
        second = jnp.minimum(jnp.maximum(first, other), jnp.minimum(second, runner))
        first = jnp.minimum(first, other)
    alive = live[...] > 0.0
    nearest[...] = jnp.where(alive, (first + query[...]) * (1.0 / width), 0.0)
    margin[...] = jnp.where(alive, (second - first) * (1.0 / width), 0.0)


def local(word_ids, word_weights, neighbours, descriptors, keypoint_count, send_table, pair_slots):
    words = lax.axis_size("word")
    subs = lax.axis_size("sub")
    w = lax.axis_index("word")
    s = lax.axis_index("sub")
    reach = words // 2
    forward = [(i, (i + 1) % words) for i in range(words)]
    backward = [(i, (i - 1) % words) for i in range(words)]
    slots, images = word_ids.shape[1:]
    topk = neighbours.shape[0]
    padded = -(-topk // 8) * 8
    per = images // (words * subs)
    held, depth, points = descriptors.shape
    half = held // 2
    targets = 2 * subs
    width = depth * subs
    pair_total = pair_slots.shape[2]

    def send(x, direction):
        return lax.ppermute(x, "word", forward if direction == 0 else backward)

    fa, ba = [send(descriptors[:half], 0)], [send(descriptors[:half], 1)]

    ids = jnp.transpose(word_ids[0].astype(F32), (1, 0))
    values = jnp.transpose(word_weights[0], (1, 0))
    table = jnp.concatenate((ids, ids, values, values), axis=1)
    mine = lax.dynamic_index_in_dim(table.reshape(words, subs, per, LANES), s, 1, keepdims=False)
    near = lax.dynamic_index_in_dim(neighbours.reshape(topk, words, subs, per), s, 2, keepdims=False)
    near = jnp.transpose(near, (1, 2, 0)).reshape(words, 1, per * topk)

    def from_here(x):
        return lax.dynamic_slice_in_dim(jnp.concatenate((x, x), axis=0), w, words, 0)

    mine_here = from_here(mine)
    near_here = from_here(near)
    table3 = table.reshape(images, 1, LANES)
    norm = call(norm_kernel, struct((2, LANES), F32), (mine.reshape(words * per, LANES),))

    def cross(k, dep):
        at_f, at_b = reach + 1 - k, (reach + k) % words
        block = lambda at: pl.BlockSpec((1, per, LANES), lambda i: (at, 0, 0))
        index = lambda at: pl.BlockSpec((1, 1, per * topk), lambda i: (at, 0, 0), memory_space=SMEM)
        return call(
            functools.partial(cross_kernel, topk),
            struct((2, 4, LANES), F32),
            (table3, mine_here, mine_here, near_here, near_here, dep),
            [vm(), block(at_f), block(at_b), index(at_f), index(at_b), pl.BlockSpec(memory_space=pl.ANY)],
            (
                pltpu.VMEM((2, 8, 8, LANES), F32),
                pltpu.VMEM((padded, LANES), F32),
                pltpu.VMEM((4 * LANES, LANES), F32),
            ),
        )

    order = [0]
    for d in range(1, reach):
        order += [words - d, d]
    order += [reach]
    source = lax.rem(w + jnp.array(order, I32), words)
    taken = lax.dynamic_index_in_dim(send_table, w, 1, keepdims=False).reshape(words, targets)[source]
    flat_taken = taken.reshape(-1)
    own_images = lax.dynamic_slice_in_dim(taken, 2 * s, 2, 1) + source[:, None] * held
    own_count = keypoint_count[own_images.reshape(-1)]
    column = jnp.arange(points, dtype=I32)[None, :]
    pen = jnp.where(column < own_count[:, None], 0.0, PENALTY).astype(F32)
    pairs = pair_slots[0, 0]
    delta = lax.rem(pairs // 2 - w + words, words)
    place = jnp.where(delta < reach, 2 * delta, 2 * (words - delta) - 1)
    pairs = place * 2 + lax.rem(pairs, 2)
    live = jnp.where(column < own_count[pairs[:, 0]][:, None], 1.0, 0.0).astype(F32)
    flat_pairs = pairs.reshape(-1)
    ahead = lax.rem(w + jnp.array([1, 2, 3, 4, words - 1, words - 2, words - 3, words - 4], I32), words)
    behind = lax.rem(w + jnp.array([words - reach + 4] * 4 + [reach - 4] * 4, I32), words)
    trims = send_table.reshape(words * words, targets)[behind * words + ahead].reshape(-1)

    listed = near_here[0].reshape(per, topk)
    listed = jnp.pad(listed, ((0, 0), (0, padded - topk)))
    itself = (w * subs + s) * per + jnp.arange(per, dtype=I32)[:, None] + jnp.zeros((1, padded), I32)

    def locate(image):
        flat = jnp.pad(image.reshape(-1), (0, 4 * LANES - per * padded)).reshape(4, LANES)
        spot = (flat // (subs * per)) * per + lax.rem(flat, per)
        return lax.rem(flat // per, subs) * 2 + spot // LANES, lax.rem(spot, LANES)

    near_row, near_lane = locate(listed)
    own_row, own_lane = locate(itself)

    block = struct((half + 1, depth, points))
    norm_struct = struct((2, LANES), F32)
    product = cross(1, descriptors)
    out_f, out_b = call(first_kernel, (block, block), (descriptors, norm, product))
    fb, bb = [send(out_f, 0)], [send(out_b, 1)]
    full = reach - 4
    arrived = []
    exchange = []
    start = 0
    sources = [(descriptors,)]
    for k in range(2, full + 1):
        fa.append(send(fa[-1], 0))
        ba.append(send(ba[-1], 1))
        product = cross(k, fa[-2])
        out_f, out_b, norm = call(
            merge_kernel, (block, block, norm_struct), (fb[-1], bb[-1], norm, product)
        )
        sources += [(fa[k - 2], fb[-1]), (ba[k - 2], bb[-1])]
        fb.append(send(out_f, 0))
        bb.append(send(out_b, 1))
        if k - 1 in GROUPS:
            exchange.append(exchange_group(sources[start:], start, flat_taken, subs, depth, points))
            start = len(sources)
    sources += [(fa[-1], fb[-1]), (ba[-1], bb[-1])]
    product = cross(full + 1, fa[-1])
    small, large = struct((targets + targets // 2, depth, points)), struct((2 * targets + 1, depth, points))
    a_f, b_f, a_b, b_b, norm = call(
        functools.partial(trim_kernel, targets),
        (small, large, small, large, norm_struct),
        (trims, fa[-1], fb[-1], ba[-1], bb[-1], norm, product),
        [sm()] + [vm()] * 6,
    )
    a_f, a_b, b_f, b_b = send(a_f, 0), send(a_b, 1), send(b_f, 0), send(b_b, 1)
    exchange.append(exchange_group(sources[start:], start, flat_taken, subs, depth, points))
    start = len(sources)
    thirteen = (a_f, a_b)
    product = cross(full + 2, a_f)
    one = struct((targets + 1, depth, points))
    a_f, b_f, a_b, b_b, norm = call(
        functools.partial(after_trim_kernel, targets),
        (one, small, one, small, norm_struct),
        (a_f, b_f, a_b, b_b, norm, product),
    )
    a_f, a_b, b_f, b_b = send(a_f, 0), send(a_b, 1), send(b_f, 0), send(b_b, 1)
    fourteen = (a_f, a_b)
    product = cross(full + 3, a_f)
    joined = struct((targets + targets // 2 + 1, depth, points))
    c_f, c_b, norm = call(
        functools.partial(join_kernel, targets),
        (joined, joined, norm_struct),
        (a_f, b_f, a_b, b_b, norm, product),
    )
    product = cross(full + 4, a_f)
    c_f, c_b = send(c_f, 0), send(c_b, 1)
    fifteen = (c_f, c_b)
    c_f, c_b, norm, dots = call(
        functools.partial(last_kernel, targets),
        (
            struct((targets // 2 + 1, depth, points)),
            struct((targets // 2, depth, points)),
            norm_struct,
            struct((4, LANES), F32),
        ),
        (c_f, c_b, norm, product),
    )
    c_f, c_b = send(c_f, 0), send(c_b, 1)
    tail, dots = call(
        functools.partial(tail_kernel, targets),
        (struct((subs, 15, depth, points)), struct((4, LANES), F32)),
        thirteen + fourteen + fifteen + (c_f, c_b, norm, dots),
    )
    exchange.append(lax.all_to_all(tail, "sub", 0, 0, tiled=True))

    counts = [x.shape[1] for x in exchange]
    counts[-1] -= 1
    total = sum(counts)
    ins = (flat_pairs, *exchange, pen, live, dots, near_row, near_lane, own_row, own_lane)
    rows = struct((pair_total, points), F32)
    nearest, margin, similarity = call(
        functools.partial(match_kernel, counts, width, topk, padded),
        (rows, rows, struct((per, topk), F32)),
        ins,
        [sm()] + [vm()] * (len(ins) - 1),
        (
            pltpu.VMEM((total, width + depth, points), BF16),
            pltpu.VMEM((total, width + depth, points), BF16),
            pltpu.VMEM((total, points), F32),
            pltpu.VMEM((pair_total, 8, points), F32),
            pltpu.VMEM((pair_total, 8, points), F32),
            pltpu.VMEM((pair_total, points), F32),
        ),
        8,
    )
    return similarity, nearest[None, None], margin[None, None]


def exchange_group(sources, start, taken, subs, depth, points):
    refs = [ref for source in sources for ref in source]
    kinds = [len(source) for source in sources]
    chosen = call(
        functools.partial(select_kernel, subs, start, kinds),
        struct((subs, 2 * len(sources), depth, points)),
        (taken, *refs),
        [sm()] + [vm()] * len(refs),
    )
    return lax.all_to_all(chosen, "sub", 0, 0, tiled=True)


def solution(mesh):
    in_specs = (
        P("word", None, "groups"),
        P("word", None, "groups"),
        P(None, "groups"),
        P(("groups", "word"), "sub", None),
        P("groups"),
        P("groups", None, None, None),
        P(("groups", "word"), "sub", None, None),
    )
    out_specs = (
        P(("groups", "word", "sub"), None),
        P(("groups", "word"), "sub", None, None),
        P(("groups", "word"), "sub", None, None),
    )
    return jax.shard_map(local, mesh=mesh, in_specs=in_specs, out_specs=out_specs, check_vma=False)
```

```python
import functools

import jax
import jax.numpy as jnp
from jax import lax
from jax.experimental import pallas as pl
from jax.experimental.pallas import tpu as pltpu
from jax.sharding import PartitionSpec as P


INTERPRET = False
F32, BF16, I32 = jnp.float32, jnp.bfloat16, jnp.int32
LANES = 128
PENALTY = 1e30
SMEM = pltpu.SMEM
VMEM = pltpu.VMEM
GROUPS = (8,)


def call(body, outs, ins, specs=None, scratch=(), mebibytes=2):
    specs = specs or [vm() for _ in ins]
    single = not isinstance(outs, (list, tuple))
    out_list = [outs] if single else list(outs)
    ins = [
        pltpu.with_memory_space_constraint(x, VMEM) if spec.memory_space is VMEM and not INTERPRET else x
        for x, spec in zip(ins, specs)
    ]
    gridded = any(spec.block_shape is not None for spec in specs)
    result = pl.pallas_call(
        body,
        out_shape=[x if INTERPRET else VMEM(x.shape, x.dtype) for x in out_list],
        in_specs=specs,
        out_specs=[vm() for _ in out_list],
        **({"grid": (1,)} if gridded else {}),
        scratch_shapes=list(scratch),
        compiler_params=pltpu.CompilerParams(vmem_limit_bytes=mebibytes << 20),
        interpret=INTERPRET,
    )(*ins)
    return result[0] if single else result


def vm():
    return pl.BlockSpec(memory_space=VMEM)


def sm():
    return pl.BlockSpec(memory_space=SMEM)


def struct(shape, dtype=BF16):
    return jax.ShapeDtypeStruct(shape, dtype)


def rounded(x):
    return x.astype(BF16).astype(F32)


def split3(x):
    first = rounded(x)
    rest = x - first
    second = rounded(rest)
    return first, second, rounded(rest - second)


def encode(norms, dots):
    high = rounded(norms)
    low = rounded(norms - high)
    return jnp.concatenate((high, low) + split3(dots), axis=0).astype(BF16)


def decode(tile):
    wide = tile.astype(F32)
    norms = wide[0:2] + wide[2:4]
    dots = (wide[4:8] + wide[8:12]) + wide[12:16]
    return norms, dots, wide[0:4]


def re_encode(head, dots):
    return jnp.concatenate((head,) + split3(dots), axis=0).astype(BF16)


def spread(rows):
    turned = pltpu.roll(rows, 64, 1)
    low = lax.broadcasted_iota(I32, rows.shape, 1) < 64
    return jnp.where(low, rows, turned), jnp.where(low, turned, rows)


def staggered(four):
    group = lax.broadcasted_iota(I32, four.shape, 1) // 32
    out = four
    for g in range(1, 4):
        out = jnp.where(group == g, pltpu.roll(four, LANES - 8 * g, 1), out)
    return out


def lane_sums(products):
    ones = jnp.ones((8, LANES), F32)
    return lax.dot_general(
        ones, products, (((1,), (1,)), ((), ())), precision=lax.Precision.HIGHEST, preferred_element_type=F32
    )


def norm_kernel(ids_ref, values_ref, out_ref):
    for j in range(out_ref.shape[0]):
        lanes = slice(j * LANES, (j + 1) * LANES)
        ids, values = ids_ref[:, lanes], values_ref[:, lanes]
        acc = jnp.zeros_like(values)
        for b in range(ids_ref.shape[0]):
            acc = acc + jnp.where(ids == ids_ref[b : b + 1, lanes], values_ref[b : b + 1, lanes], 0.0)
        out_ref[j : j + 1, :] = jnp.sum(acc * values, axis=0, keepdims=True)


def cross_kernel(count, table_ref, rows_f, rows_b, idx_f, idx_b, dep_ref, out_ref, turned, gathered, products):
    del dep_ref
    padded = gathered.shape[0]
    images = rows_f.shape[1]
    gathered[...] = jnp.zeros_like(gathered)
    products[...] = jnp.zeros_like(products)
    for which, (rows_ref, idx_ref) in enumerate(((rows_f, idx_f), (rows_b, idx_b))):
        ids, weights = spread(rows_ref[0])
        other, value = staggered(ids), staggered(weights)
        for t in range(8):
            turned[0, t] = pltpu.roll(other, LANES - t, 1) if t else other
            turned[1, t] = pltpu.roll(value, LANES - t, 1) if t else value

        def image(i, carry):
            for k in range(count):
                row = idx_ref[0, 0, i * count + k]
                gathered[k : k + 1, :] = table_ref[row]
            queries = [turned[0, t, pl.ds(i, 1), :] for t in range(8)]
            scales = [turned[1, t, pl.ds(i, 1), :] for t in range(8)]
            for part in range(padded // 8):
                near_ids, near_weights = spread(gathered[part * 8 : part * 8 + 8, :])
                acc = jnp.zeros_like(near_ids)
                for t in range(8):
                    acc = acc + jnp.where(near_ids == queries[t], scales[t], 0.0)
                start = pl.multiple_of(i * padded + part * 8, 8)
                products[pl.ds(start, 8), :] = acc * near_weights
            return carry

        lax.fori_loop(0, images, image, 0)
        sums = lane_sums(products[...])
        for j in range(4):
            out_ref[which, j : j + 1, :] = sums[0:1, j * LANES : (j + 1) * LANES]


def first_kernel(desc_ref, norm_ref, cross_ref, out):
    held = desc_ref.shape[0]
    out[0:held] = desc_ref[...]
    for e in range(2):
        out[held + e] = encode(norm_ref[2 * e : 2 * e + 2], cross_ref[e])


def merge_kernel(skip, recv, norm_ref, cross_ref, out, norm_out):
    kept = out.shape[0] - 2
    last = recv.shape[0] - 2
    out[0:kept] = recv[skip : skip + kept]
    for e in range(2):
        norms, dots, head = decode(recv[last + e])
        out[kept + e] = re_encode(head, dots + cross_ref[e])
        norm_out[2 * e : 2 * e + 2] = norm_ref[2 * e : 2 * e + 2] + norms


def trim_kernel(idx, recv_a, recv_b, norm_ref, cross_ref, out_a, out_b, norm_out):
    kept = out_a.shape[0]
    last = recv_b.shape[0] - 2
    for n in range(kept):
        out_a[n] = recv_a[idx[n]]
        out_b[n] = recv_b[idx[n]]
    for e in range(2):
        norms, dots, head = decode(recv_b[last + e])
        out_b[kept + e] = re_encode(head, dots + cross_ref[e])
        norm_out[2 * e : 2 * e + 2] = norm_ref[2 * e : 2 * e + 2] + norms


def select_kernel(subs, distances, info, idx, *refs):
    out = refs[-1]
    core = info[0]
    at = 0
    step = 0
    for d in distances:
        row = 2 * d - 1 + core if d else 0
        for s in range(subs):
            for c in range(2):
                slot = idx[row * 2 * subs + s * 2 + c]
                if d:
                    out[s, 4 * step + 2 * c + core] = refs[at][slot]
                    out[s, 4 * step + 2 * c + 1 - core] = refs[at + 1][slot]
                else:
                    out[s, 4 * (len(distances) - 1) + c] = refs[at][slot]
        at += 2 if d else 1
        step += 1 if d else 0


def tail_kernel(subs, info, *refs):
    blocks, (norm_ref, kept_ref, out) = refs[:-3], refs[-3:]
    core = info[0]
    last = len(blocks) // 2 - 1
    for j in range(last + 1):
        for q, src in ((core, blocks[2 * j]), (1 - core, blocks[2 * j + 1])):
            for s in range(subs):
                for c in range(2):
                    slot = 2 * s + c if j < last else 2 * (s % (subs // 2)) + c
                    out[s, 4 * j + 2 * c + q] = src[slot]
    recv = blocks[-1]
    size = recv.shape[0] - 2
    upward = core == 0
    totals = []
    empty = jnp.zeros((4, LANES), F32)
    for e in range(2):
        norms, dots, _ = decode(recv[size + e])
        totals.append(norm_ref[2 * e : 2 * e + 2] + jnp.where(upward, norms, 0.0))
        own = jnp.where(upward, dots, kept_ref[e])
        tile = jnp.concatenate(split3(own) + (empty,), axis=0).astype(BF16)
        for s in range(subs // 2):
            out[2 * s + e, 4 * last + 5] = tile
    tile = jnp.concatenate(split3(jnp.concatenate(totals, axis=0)) + (empty,), axis=0).astype(BF16)
    for s in range(subs):
        out[s, 4 * last + 4] = tile


def keep_kernel(recv, cross_ref, out):
    last = recv.shape[0] - 2
    for e in range(2):
        _, dots, _ = decode(recv[last + e])
        out[e] = dots + cross_ref[e]


def joined(tile):
    wide = tile.astype(F32)
    return (wide[0:4] + wide[4:8]) + wide[8:12]


def match_kernel(count, plan, width, topk, padded, pairs, info, *refs):
    groups = refs[:count]
    pen, live, near_row, near_lane, own_row, own_lane = refs[count : count + 6]
    nearest, margin, similarity = refs[count + 6 : count + 9]
    lhs, rhs, squares, least, less, query = refs[count + 9 :]
    pair_total = nearest.shape[0]
    subs = groups[0].shape[0]
    depth = groups[0].shape[2]
    wide = subs * depth
    end = groups[-1].shape[1]

    near = jnp.zeros(near_row.shape, F32)
    own = jnp.zeros(near_row.shape, F32)
    for x in range(subs // 2):
        rows = joined(groups[-1][2 * x, end - 2]) + joined(groups[-1][2 * x + 1, end - 2])
        for h in range(4):
            line = jnp.broadcast_to(rows[h : h + 1], near_row.shape)
            at = jnp.take_along_axis(line, near_lane[...], axis=1)
            near = jnp.where(near_row[...] == 4 * x + h, at, near)
            at = jnp.take_along_axis(line, own_lane[...], axis=1)
            own = jnp.where(own_row[...] == 4 * x + h, at, own)
    chip = info[1]
    dots = joined(groups[-1][2 * chip, end - 1]) + joined(groups[-1][2 * chip + 1, end - 1])
    cosine = dots / jnp.sqrt(own * near)
    for r in range(similarity.shape[0]):
        line, lane = divmod(r * padded, LANES)
        both = jnp.concatenate((cosine[line : line + 1], cosine[line + 1 : line + 2]), axis=1) if line < 3 else cosine[3:4]
        similarity[r : r + 1, :] = both[:, lane : lane + topk]

    tail = rhs.shape[1] - wide
    row = lax.broadcasted_iota(I32, (tail, LANES), 0)
    ones = jnp.where(row < 4, 1.0, 0.0).astype(BF16)

    def prepare(slot, blocks):
        total = jnp.zeros((depth, LANES), F32)
        for s, block in enumerate(blocks):
            rhs[slot, s * depth : (s + 1) * depth, :] = block
            value = block.astype(F32)
            lhs[slot, s * depth : (s + 1) * depth, :] = (value * -2.0).astype(BF16)
            total = total + value * value
        square = jnp.sum(total, axis=0, keepdims=True)
        squares[pl.ds(slot, 1), :] = square
        parts = split3(square)
        extra = jnp.where(row == 0, parts[0], 0.0)
        extra = jnp.where(row == 1, parts[1], extra)
        extra = jnp.where(row == 2, parts[2], extra)
        extra = jnp.where(row == 3, pen[pl.ds(slot, 1), :], extra)
        lhs[slot, wide:, :] = extra.astype(BF16)
        rhs[slot, wide:, :] = ones

    for which, first, positions, ways, at in plan:
        group = groups[which]

        def image(i, carry, group=group, first=first, ways=ways, at=at):
            if ways == 0:
                prepare(i, [group[s, at + i] for s in range(subs)])
                return carry
            source = i // 2
            step = source // ways
            lineage = source - ways * step if ways == 2 else info[2]
            tile = at + 4 * step + 2 * (i - 2 * source)
            prepare(2 * first + i, [group[2 * (s // 2) + lineage, tile + s % 2] for s in range(subs)])
            return carry

        lax.fori_loop(0, 2 * positions, image, 0)

    def pair(p, carry):
        asked = pairs[2 * p]
        refer = pairs[2 * p + 1]
        scores = lax.dot_general(
            lhs[refer], rhs[asked], (((0,), (0,)), ((), ())), preferred_element_type=F32
        )
        first = scores[0:8]
        second = jnp.full_like(first, PENALTY)
        for b in range(1, LANES // 8):
            value = scores[8 * b : 8 * b + 8]
            second = jnp.minimum(second, jnp.maximum(first, value))
            first = jnp.minimum(first, value)
        least[p] = first
        less[p] = second
        query[pl.ds(p, 1), :] = squares[pl.ds(asked, 1), :]
        return carry

    lax.fori_loop(0, pair_total, pair, 0)
    first = least[:, 0, :]
    second = less[:, 0, :]
    for b in range(1, 8):
        other, runner = least[:, b, :], less[:, b, :]
        second = jnp.minimum(jnp.maximum(first, other), jnp.minimum(second, runner))
        first = jnp.minimum(first, other)
    alive = live[...] > 0.0
    nearest[...] = jnp.where(alive, (first + query[...]) * (1.0 / width), 0.0)
    margin[...] = jnp.where(alive, (second - first) * (1.0 / width), 0.0)


def local(word_ids, word_weights, neighbours, descriptors, keypoint_count, send_table, pair_slots):
    words = lax.axis_size("word")
    subs = lax.axis_size("sub")
    w = lax.axis_index("word")
    s = lax.axis_index("sub")
    core = lax.rem(s, 2)
    reach = words // 2
    pairs_of_ring = [
        (i * subs + j, ((i + (1 if j % 2 == 0 else words - 1)) % words) * subs + j)
        for i in range(words)
        for j in range(subs)
    ]
    _, images = word_ids.shape[1:]
    topk = neighbours.shape[0]
    padded = -(-topk // 8) * 8
    per = images // (words * subs)
    held, depth, points = descriptors.shape
    targets = 2 * subs
    width = depth * subs
    pair_total = pair_slots.shape[2]

    def send(x):
        return lax.ppermute(x, ("word", "sub"), pairs_of_ring)

    a = send(descriptors)
    partner = lax.ppermute(descriptors, "sub", [(j, j ^ 1) for j in range(subs)])

    wide_ids = word_ids[0].astype(F32)
    ids = jnp.transpose(wide_ids, (1, 0))
    values = jnp.transpose(word_weights[0], (1, 0))
    table = jnp.concatenate((ids, ids, values, values), axis=1)
    chips = subs // 2
    chip = s // 2
    mine = lax.dynamic_index_in_dim(table.reshape(words, chips, 2 * per, LANES), chip, 1, keepdims=False)
    near = lax.dynamic_index_in_dim(neighbours.reshape(topk, words, chips, 2 * per), chip, 2, keepdims=False)
    near = jnp.transpose(near, (1, 2, 0)).reshape(words, 2 * per * topk)
    count = jnp.arange(1, reach + 1, dtype=I32)
    turn = lax.rem(w + jnp.where(core == 0, reach + 1 - count, reach + count), words)
    mine_order = mine[turn].reshape(2 * reach, per, LANES)
    near_order = near[turn].reshape(2 * reach, 1, per * topk)
    table3 = table.reshape(images, 1, LANES)
    share = images // chips
    norm = call(
        norm_kernel,
        struct((share // LANES, LANES), F32),
        (
            lax.dynamic_slice_in_dim(wide_ids, chip * share, share, 1),
            lax.dynamic_slice_in_dim(word_weights[0], chip * share, share, 1),
        ),
    )

    def cross(k, dep):
        block = lambda e: pl.BlockSpec((1, per, LANES), lambda i: (2 * k - 2 + e, 0, 0))
        index = lambda e: pl.BlockSpec((1, 1, per * topk), lambda i: (2 * k - 2 + e, 0, 0), memory_space=SMEM)
        return call(
            functools.partial(cross_kernel, topk),
            struct((2, 4, LANES), F32),
            (table3, mine_order, mine_order, near_order, near_order, dep),
            [vm(), block(0), block(1), index(0), index(1), vm()],
            (
                pltpu.VMEM((2, 8, 8, LANES), F32),
                pltpu.VMEM((padded, LANES), F32),
                pltpu.VMEM((4 * LANES, LANES), F32),
            ),
        )

    order = [0]
    for d in range(1, reach):
        order += [words - d, d]
    order += [reach]
    source = lax.rem(w + jnp.array(order, I32), words)
    taken = lax.dynamic_index_in_dim(send_table, w, 1, keepdims=False).reshape(words, targets)[source]
    flat_taken = taken.reshape(-1)
    own_images = lax.dynamic_slice_in_dim(taken, 2 * s, 2, 1) + source[:, None] * held
    own_count = keypoint_count[own_images.reshape(-1)]
    column = jnp.arange(points, dtype=I32)[None, :]
    pen = jnp.where(column < own_count[:, None], 0.0, PENALTY).astype(F32)
    pairs = pair_slots[0, 0]
    delta = lax.rem(pairs // 2 - w + words, words)
    place = jnp.where(delta < reach, 2 * delta, 2 * (words - delta) - 1)
    pairs = place * 2 + lax.rem(pairs, 2)
    live = jnp.where(column < own_count[pairs[:, 0]][:, None], 1.0, 0.0).astype(F32)
    flat_pairs = pairs.reshape(-1)
    sign = 1 - 2 * core
    ahead = lax.rem(w + sign * jnp.arange(1, 5, dtype=I32) + words, words)
    behind = lax.rem(w - sign * (reach - 4) + words, words)
    trims = lax.dynamic_index_in_dim(send_table, behind, 0, keepdims=False).reshape(words, targets)[ahead]
    trims = jnp.concatenate((trims[:3].reshape(-1), lax.dynamic_slice_in_dim(trims[3], core * subs, subs, 0)))
    info = jnp.stack((core, chip, s // chips, core)).astype(I32)

    at_own = (w * subs + s) * per
    listed = jnp.transpose(lax.dynamic_slice_in_dim(neighbours, at_own, per, 1), (1, 0))
    listed = jnp.pad(listed, ((0, 0), (0, padded - topk)))
    itself = at_own + jnp.arange(per, dtype=I32)[:, None] + jnp.zeros((1, padded), I32)

    def locate(image):
        flat = jnp.pad(image.reshape(-1), (0, 4 * LANES - per * padded)).reshape(4, LANES)
        return flat // LANES, lax.rem(flat, LANES)

    near_row, near_lane = locate(listed)
    own_row, own_lane = locate(itself)

    def select(distances, blocks):
        refs = [block for pair in blocks for block in pair]
        own = 2 if distances[0] == 0 else 0
        chosen = call(
            functools.partial(select_kernel, subs, distances),
            struct((subs, 4 * (len(distances) - own // 2) + own, depth, points)),
            (info, flat_taken, *refs),
            [sm(), sm()] + [vm()] * len(refs),
        )
        return lax.all_to_all(chosen, "sub", 0, 0, tiled=True)

    norm_struct = struct((share // LANES, LANES), F32)
    first = (partner, norm, cross(1, descriptors))
    b = send(call(first_kernel, struct((held + 2, depth, points)), first))
    norm = jnp.where(core == 0, norm, 0.0)
    blocks = [(descriptors,), (a, b)]
    exchange = []
    plan = []
    start = 0
    full = reach - 4

    def deliver(stop):
        plan.append((len(exchange), max(2 * start - 1, 1), 2 * (stop - max(start, 1) + 1), 2, 0))
        if start == 0:
            plan.append((0, 0, 1, 0, 4 * stop))
        exchange.append(select(list(range(start, stop + 1)), blocks[start : stop + 1]))

    for k in range(2, full + 1):
        product = cross(k, a)
        a = send(a)
        merged, norm = call(
            functools.partial(merge_kernel, 0), (struct((held + 2, depth, points)), norm_struct), (b, norm, product)
        )
        b = send(merged)
        if k - 1 in GROUPS:
            deliver(k - 1)
            start = k
        blocks.append((a, b))
    size = 3 * targets + subs
    a, b, norm = call(
        trim_kernel,
        (struct((size, depth, points)), struct((size + 2, depth, points)), norm_struct),
        (trims, a, b, norm, cross(full + 1, a)),
        [sm()] + [vm()] * 4,
    )
    a, b = send(a), send(b)
    deliver(full)
    last = [a, b]
    for k in range(full + 2, reach + 1):
        size -= targets
        product = cross(k, a)
        if k == reach:
            kept = call(keep_kernel, struct((2, 4, LANES), F32), (b, product))
        a = send(a[targets:])
        merged, norm = call(
            functools.partial(merge_kernel, targets),
            (struct((size + 2, depth, points)), norm_struct),
            (b, norm, product),
        )
        b = send(merged)
        last += [a, b]
    steps = len(last) // 2
    tail = call(
        functools.partial(tail_kernel, subs),
        struct((subs, 4 * steps + 2, depth, points)),
        (info, *last, norm, kept),
        [sm()] + [vm()] * (len(last) + 2),
    )
    plan.append((len(exchange), 2 * full + 1, 2 * (steps - 1), 2, 0))
    plan.append((len(exchange), 2 * reach - 1, 1, 1, 4 * (steps - 1)))
    exchange.append(lax.all_to_all(tail, "sub", 0, 0, tiled=True))

    total = 2 * words
    ins = (flat_pairs, info, *exchange, pen, live, near_row, near_lane, own_row, own_lane)
    rows = struct((pair_total, points), F32)
    nearest, margin, similarity = call(
        functools.partial(match_kernel, len(exchange), plan, width, topk, padded),
        (rows, rows, struct((per, topk), F32)),
        ins,
        [sm(), sm()] + [vm()] * (len(ins) - 2),
        (
            pltpu.VMEM((total, width + depth, points), BF16),
            pltpu.VMEM((total, width + depth, points), BF16),
            pltpu.VMEM((total, points), F32),
            pltpu.VMEM((pair_total, 8, points), F32),
            pltpu.VMEM((pair_total, 8, points), F32),
            pltpu.VMEM((pair_total, points), F32),
        ),
        8,
    )
    return similarity, nearest[None, None], margin[None, None]


def solution(mesh):
    in_specs = (
        P("word", None, "groups"),
        P("word", None, "groups"),
        P(None, "groups"),
        P(("groups", "word"), "sub", None),
        P("groups"),
        P("groups", None, None, None),
        P(("groups", "word"), "sub", None, None),
    )
    out_specs = (
        P(("groups", "word", "sub"), None),
        P(("groups", "word"), "sub", None, None),
        P(("groups", "word"), "sub", None, None),
    )

    return jax.shard_map(local, mesh=mesh, in_specs=in_specs, out_specs=out_specs, check_vma=False)
```

```python
import functools

import jax
import jax.numpy as jnp
from jax import lax
from jax.experimental import pallas as pl
from jax.experimental.pallas import tpu as pltpu
from jax.sharding import PartitionSpec as P


INTERPRET = False
F32, BF16, I32 = jnp.float32, jnp.bfloat16, jnp.int32
LANES = 128
PENALTY = 1e30
SMEM = pltpu.SMEM
VMEM = pltpu.VMEM
GROUPS = (8,)


def call(body, outs, ins, specs=None, scratch=(), mebibytes=2, aliases=None, outside=()):
    specs = specs or [vm() for _ in ins]
    single = not isinstance(outs, (list, tuple))
    out_list = [outs] if single else list(outs)
    ins = [
        pltpu.with_memory_space_constraint(x, VMEM) if spec.memory_space is VMEM and not INTERPRET else x
        for x, spec in zip(ins, specs)
    ]
    gridded = any(spec.block_shape is not None for spec in specs)
    result = pl.pallas_call(
        body,
        out_shape=[x if INTERPRET or i in outside else VMEM(x.shape, x.dtype) for i, x in enumerate(out_list)],
        in_specs=specs,
        out_specs=[pl.BlockSpec(memory_space=pl.ANY) if i in outside else vm() for i in range(len(out_list))],
        **({"grid": (1,)} if gridded else {}),
        scratch_shapes=list(scratch),
        input_output_aliases=aliases or {},
        compiler_params=pltpu.CompilerParams(vmem_limit_bytes=mebibytes << 20),
        interpret=INTERPRET,
    )(*ins)
    return result[0] if single else result


def vm():
    return pl.BlockSpec(memory_space=VMEM)


def sm():
    return pl.BlockSpec(memory_space=SMEM)


def struct(shape, dtype=BF16):
    return jax.ShapeDtypeStruct(shape, dtype)


def rounded(x):
    return x.astype(BF16).astype(F32)


def split3(x):
    first = rounded(x)
    rest = x - first
    second = rounded(rest)
    return first, second, rounded(rest - second)


def encode(norms, dots):
    high = rounded(norms)
    low = rounded(norms - high)
    return jnp.concatenate((high, low) + split3(dots), axis=0).astype(BF16)


def decode(tile):
    wide = tile.astype(F32)
    norms = wide[0:2] + wide[2:4]
    dots = (wide[4:8] + wide[8:12]) + wide[12:16]
    return norms, dots, wide[0:4]


def re_encode(head, dots):
    return jnp.concatenate((head,) + split3(dots), axis=0).astype(BF16)


def spread(rows):
    turned = pltpu.roll(rows, 64, 1)
    low = lax.broadcasted_iota(I32, rows.shape, 1) < 64
    return jnp.where(low, rows, turned), jnp.where(low, turned, rows)


def staggered(four):
    group = lax.broadcasted_iota(I32, four.shape, 1) // 32
    out = four
    for g in range(1, 4):
        out = jnp.where(group == g, pltpu.roll(four, LANES - 8 * g, 1), out)
    return out


def lane_sums(products):
    ones = jnp.ones((8, LANES), BF16)
    total = None
    for term in split3(products):
        part = lax.dot_general(ones, term.astype(BF16), (((1,), (1,)), ((), ())), preferred_element_type=F32)
        total = part if total is None else total + part
    return total


def table_kernel(info, ids_ref, values_ref, table_ref, norm_ref):
    occurrences, images = ids_ref.shape
    for j in range(images // LANES):
        lanes = slice(j * LANES, (j + 1) * LANES)
        ids, values = ids_ref[:, lanes].astype(F32), values_ref[:, lanes]
        table_ref[lanes, :] = jnp.concatenate((ids, ids, values, values), axis=0).T
    share = norm_ref.shape[0]
    for j in range(share):
        start = pl.multiple_of((info[1] * share + j) * LANES, LANES)
        ids, values = ids_ref[:, pl.ds(start, LANES)], values_ref[:, pl.ds(start, LANES)]
        acc = jnp.zeros_like(values)
        for b in range(occurrences):
            acc = acc + jnp.where(ids == ids[b : b + 1], values[b : b + 1], 0.0)
        norm_ref[j : j + 1, :] = jnp.sum(acc * values, axis=0, keepdims=True)


def cross_kernel(count, k, turn, words, chosen, info, lists, table_ref, rows_ref, *refs):
    idx, arrived, picked, stored = refs[-4:]
    refs = refs[:-4]
    fetch = pltpu.make_async_copy(lists.at[k - 1], idx, arrived)
    fetch.start()
    if chosen is None:
        out_ref, turned, gathered, products = refs
    else:
        distance, step, paired, fresh = chosen
        taken, refs = refs[0], refs[1:]
        blocks, refs = refs[: 1 + paired], refs[1 + paired + (not fresh) :]
        out_ref, group_ref, turned, gathered, products = refs
        core = info[0]
        for s in range(picked.shape[0]):
            for c in range(2):
                slot = taken[distance * 2 * picked.shape[0] + 2 * s + c]
                if paired:
                    picked[s, 2 * c + core] = blocks[0][slot]
                    picked[s, 2 * c + 1 - core] = blocks[1][slot]
                else:
                    picked[s, c] = blocks[0][slot]
        tiles = 2 + 2 * paired
        store = pltpu.make_async_copy(picked.at[:, 0:tiles], group_ref.at[:, step : step + tiles], stored)
        store.start()
    padded = gathered.shape[1]
    total = turned.shape[2]
    half = total // 2
    up, down = turn
    target = lax.rem(info[3] + jnp.where(info[0] == 0, up, down), words)
    start = pl.multiple_of((target * (rows_ref.shape[0] // (words * total)) + info[1]) * total, total)
    ids, weights = spread(rows_ref[pl.ds(start, total), :])
    other, value = staggered(ids), staggered(weights)
    for t in range(8):
        turned[0, t] = pltpu.roll(other, LANES - t, 1) if t else other
        turned[1, t] = pltpu.roll(value, LANES - t, 1) if t else value
    empty = jnp.zeros((8, LANES), F32)
    for e in range(2):
        gathered[e, padded - 8 :, :] = empty
        for part in range(half * padded // 8, 4 * LANES // 8):
            products[e, part * 8 : part * 8 + 8, :] = empty

    fetch.wait()

    def image(i, carry):
        for e in range(2):
            for k in range(count):
                row = idx[0, (e * half + i) * count + k]
                gathered[e, k : k + 1, :] = table_ref[row]
        for e in range(2):
            queries = [turned[0, t, pl.ds(e * half + i, 1), :] for t in range(8)]
            scales = [turned[1, t, pl.ds(e * half + i, 1), :] for t in range(8)]
            for part in range(padded // 8):
                near_ids, near_weights = spread(gathered[e, part * 8 : part * 8 + 8, :])
                acc = jnp.zeros_like(near_ids)
                for t in range(8):
                    acc = acc + jnp.where(near_ids == queries[t], scales[t], 0.0)
                at = pl.multiple_of(i * padded + part * 8, 8)
                products[e, pl.ds(at, 8), :] = acc * near_weights
        return carry

    lax.fori_loop(0, half, image, 0)
    for e in range(2):
        sums = lane_sums(products[e])
        for j in range(4):
            out_ref[e, j : j + 1, :] = sums[0:1, j * LANES : (j + 1) * LANES]
    if chosen is not None:
        store.wait()


def first_kernel(desc_ref, norm_ref, cross_ref, out):
    held = desc_ref.shape[0]
    out[0:held] = desc_ref[...]
    for e in range(2):
        out[held + e] = encode(norm_ref[2 * e : 2 * e + 2], cross_ref[e])


def merge_kernel(skip, recv, norm_ref, cross_ref, out, norm_out):
    kept = out.shape[0] - 2
    last = recv.shape[0] - 2
    out[0:kept] = recv[skip : skip + kept]
    for e in range(2):
        norms, dots, head = decode(recv[last + e])
        out[kept + e] = re_encode(head, dots + cross_ref[e])
        norm_out[2 * e : 2 * e + 2] = norm_ref[2 * e : 2 * e + 2] + norms


def trim_kernel(idx, recv_a, recv_b, norm_ref, cross_ref, out_a, out_b, norm_out):
    kept = out_a.shape[0]
    last = recv_b.shape[0] - 2
    for n in range(kept):
        out_a[n] = recv_a[idx[n]]
        out_b[n] = recv_b[idx[n]]
    for e in range(2):
        norms, dots, head = decode(recv_b[last + e])
        out_b[kept + e] = re_encode(head, dots + cross_ref[e])
        norm_out[2 * e : 2 * e + 2] = norm_ref[2 * e : 2 * e + 2] + norms


def tail_kernel(subs, info, *refs):
    blocks, (norm_ref, kept_ref, out) = refs[:-3], refs[-3:]
    core = info[0]
    last = len(blocks) // 2 - 1
    for j in range(last + 1):
        for q, src in ((core, blocks[2 * j]), (1 - core, blocks[2 * j + 1])):
            for s in range(subs):
                for c in range(2):
                    slot = 2 * s + c if j < last else 2 * (s % (subs // 2)) + c
                    out[s, 4 * j + 2 * c + q] = src[slot]
    recv = blocks[-1]
    size = recv.shape[0] - 2
    upward = core == 0
    totals = []
    empty = jnp.zeros((4, LANES), F32)
    for e in range(2):
        norms, dots, _ = decode(recv[size + e])
        totals.append(norm_ref[2 * e : 2 * e + 2] + jnp.where(upward, norms, 0.0))
        own = jnp.where(upward, dots, kept_ref[e])
        tile = jnp.concatenate(split3(own) + (empty,), axis=0).astype(BF16)
        for s in range(subs // 2):
            out[2 * s + e, 4 * last + 5] = tile
    tile = jnp.concatenate(split3(jnp.concatenate(totals, axis=0)) + (empty,), axis=0).astype(BF16)
    for s in range(subs):
        out[s, 4 * last + 4] = tile


def keep_kernel(recv, cross_ref, out):
    last = recv.shape[0] - 2
    for e in range(2):
        _, dots, _ = decode(recv[last + e])
        out[e] = dots + cross_ref[e]


def joined(tile):
    wide = tile.astype(F32)
    return (wide[0:4] + wide[4:8]) + wide[8:12]


def operands(plan, info, groups, pen, lhs, rhs, squares):
    subs = groups[0].shape[0]
    depth = groups[0].shape[2]
    row = lax.broadcasted_iota(I32, (depth, LANES), 0)
    ones = jnp.where(row < 4, 1.0, 0.0).astype(BF16)

    def prepare(slot, blocks):
        total = jnp.zeros((depth, LANES), F32)
        scaled = []
        for s, block in enumerate(blocks):
            rhs[slot, s * depth : (s + 1) * depth, :] = block
            value = block.astype(F32)
            scaled.append(value * -2.0)
            total = total + value * value
        square = jnp.sum(total, axis=0, keepdims=True)
        squares[pl.ds(slot, 1), :] = square
        parts = split3(square)
        extra = jnp.where(row == 0, parts[0], 0.0)
        extra = jnp.where(row == 1, parts[1], extra)
        extra = jnp.where(row == 2, parts[2], extra)
        scaled.append(jnp.where(row == 3, pen[pl.ds(slot, 1), :], extra))
        rhs[slot, subs * depth :, :] = ones
        lhs[slot] = jnp.concatenate(scaled, axis=0).T.astype(BF16)

    for which, first, positions, ways, at in plan:
        group = groups[which]

        def image(i, carry, group=group, first=first, ways=ways, at=at):
            if ways == 0:
                prepare(i, [group[s, at + i] for s in range(subs)])
                return carry
            source = i // 2
            step = source // ways
            lineage = source - ways * step if ways == 2 else info[2]
            tile = at + 4 * step + 2 * (i - 2 * source)
            prepare(2 * first + i, [group[2 * (s // 2) + lineage, tile + s % 2] for s in range(subs)])
            return carry

        lax.fori_loop(0, 2 * positions, image, 0)


def early_kernel(count, plan, info, *refs):
    pen, lhs, rhs, squares = refs[count:]
    operands(plan, info, refs[:count], pen, lhs, rhs, squares)


def joined(tile):
    wide = tile.astype(F32)
    return (wide[0:4] + wide[4:8]) + wide[8:12]


def match_kernel(plan, width, topk, padded, pairs, info, *refs):
    group, pen, live, near_row, near_lane, own_row, own_lane = refs[:7]
    nearest, margin, similarity, lhs, rhs, squares, least, less, query = refs[10:]
    pair_total = nearest.shape[0]
    subs = group.shape[0]
    end = group.shape[1]
    operands(plan, info, [group], pen, lhs, rhs, squares)

    near = jnp.zeros(near_row.shape, F32)
    own = jnp.zeros(near_row.shape, F32)
    for x in range(subs // 2):
        rows = joined(group[2 * x, end - 2]) + joined(group[2 * x + 1, end - 2])
        for h in range(4):
            line = jnp.broadcast_to(rows[h : h + 1], near_row.shape)
            at = jnp.take_along_axis(line, near_lane[...], axis=1)
            near = jnp.where(near_row[...] == 4 * x + h, at, near)
            at = jnp.take_along_axis(line, own_lane[...], axis=1)
            own = jnp.where(own_row[...] == 4 * x + h, at, own)
    chip = info[1]
    dots = joined(group[2 * chip, end - 1]) + joined(group[2 * chip + 1, end - 1])
    cosine = dots / jnp.sqrt(own * near)
    for r in range(similarity.shape[0]):
        line, lane = divmod(r * padded, LANES)
        both = jnp.concatenate((cosine[line : line + 1], cosine[line + 1 : line + 2]), axis=1) if line < 3 else cosine[3:4]
        similarity[r : r + 1, :] = both[:, lane : lane + topk]

    def pair(p, carry):
        asked = pairs[2 * p]
        refer = pairs[2 * p + 1]
        scores = jnp.dot(lhs[refer], rhs[asked], preferred_element_type=F32)
        first = scores[0:8]
        second = jnp.full_like(first, PENALTY)
        for b in range(1, LANES // 8):
            value = scores[8 * b : 8 * b + 8]
            second = jnp.minimum(second, jnp.maximum(first, value))
            first = jnp.minimum(first, value)
        least[p] = first
        less[p] = second
        query[pl.ds(p, 1), :] = squares[pl.ds(asked, 1), :]
        return carry

    def four(q, carry):
        for r in range(4):
            pair(4 * q + r, carry)
        return carry

    if pair_total % 4 == 0:
        lax.fori_loop(0, pair_total // 4, four, 0)
    else:
        lax.fori_loop(0, pair_total, pair, 0)
    first = least[:, 0, :]
    second = less[:, 0, :]
    for b in range(1, 8):
        other, runner = least[:, b, :], less[:, b, :]
        second = jnp.minimum(jnp.maximum(first, other), jnp.minimum(second, runner))
        first = jnp.minimum(first, other)
    alive = live[...] > 0.0
    nearest[...] = jnp.where(alive, (first + query[...]) * (1.0 / width), 0.0)
    margin[...] = jnp.where(alive, (second - first) * (1.0 / width), 0.0)


def local(word_ids, word_weights, neighbours, descriptors, keypoint_count, send_table, pair_slots):
    words = lax.axis_size("word")
    subs = lax.axis_size("sub")
    w = lax.axis_index("word")
    s = lax.axis_index("sub")
    core = lax.rem(s, 2)
    reach = words // 2
    pairs_of_ring = [
        (i * subs + j, ((i + (1 if j % 2 == 0 else words - 1)) % words) * subs + j)
        for i in range(words)
        for j in range(subs)
    ]
    _, images = word_ids.shape[1:]
    topk = neighbours.shape[0]
    padded = -(-topk // 8) * 8
    per = images // (words * subs)
    held, depth, points = descriptors.shape
    targets = 2 * subs
    width = depth * subs
    pair_total = pair_slots.shape[2]

    def send(x):
        return lax.ppermute(x, ("word", "sub"), pairs_of_ring)

    a = send(descriptors)
    partner = lax.ppermute(descriptors, "sub", [(j, j ^ 1) for j in range(subs)])

    chips = subs // 2
    chip = s // 2
    info = jnp.stack((core, chip, s // chips, w)).astype(I32)
    share = images // chips // LANES
    table, norm = call(
        table_kernel,
        (struct((images, LANES), F32), struct((share, LANES), F32)),
        (info, word_ids[0], word_weights[0]),
        [sm(), vm(), vm()],
        (),
        4,
    )
    table3 = table.reshape(images, 1, LANES)
    near = lax.dynamic_index_in_dim(neighbours.reshape(topk, words, chips, 2 * per), chip, 2, keepdims=False)
    near = jnp.transpose(near, (1, 2, 0)).reshape(words, 2 * per * topk)
    count = jnp.arange(1, reach + 1, dtype=I32)
    turn = lax.rem(w + jnp.where(core == 0, reach + 1 - count, reach + count), words)
    near_order = near[turn].reshape(reach, 1, 2 * per * topk)
    away = jnp.arange(0, reach, dtype=I32)
    taken_here = lax.dynamic_index_in_dim(send_table, w, 1, keepdims=False).reshape(words, targets)
    taken_mine = taken_here[lax.rem(w + jnp.where(core == 0, words - away, away), words)].reshape(-1)

    def cross(k, distance=None, sources=(), group=None, step=0, tiles=0):
        specs = [sm(), pl.BlockSpec(memory_space=pl.ANY), vm(), vm()]
        ins = [info, near_order, table3, table]
        outs = [struct((2, 4, LANES), F32)]
        chosen, aliases = None, {}
        if sources:
            chosen = (distance, step, len(sources) - 1, group is None)
            specs += [sm()]
            ins += [taken_mine, *sources]
            specs += [vm()] * len(sources)
            outs += [struct((subs, tiles, depth, points))]
            if group is not None:
                aliases = {len(ins): 1}
                ins += [group]
                specs += [pl.BlockSpec(memory_space=pl.ANY)]
        result = call(
            functools.partial(cross_kernel, topk, k, (reach + 1 - k, reach + k), words, chosen),
            outs,
            ins,
            specs,
            (
                pltpu.VMEM((2, 8, 2 * per, LANES), F32),
                pltpu.VMEM((2, padded, LANES), F32),
                pltpu.VMEM((2, 4 * LANES, LANES), F32),
                pltpu.SMEM((1, 2 * per * topk), I32),
                pltpu.SemaphoreType.DMA(()),
                pltpu.VMEM((subs, 4, depth, points), BF16),
                pltpu.SemaphoreType.DMA(()),
            ),
            4,
            aliases,
            {1},
        )
        return result if sources else result[0]

    order = [0]
    for d in range(1, reach):
        order += [words - d, d]
    order += [reach]
    source = lax.rem(w + jnp.array(order, I32), words)
    taken = taken_here[source]
    own_images = lax.dynamic_slice_in_dim(taken, 2 * s, 2, 1) + source[:, None] * held
    own_count = keypoint_count[own_images.reshape(-1)]
    column = jnp.arange(points, dtype=I32)[None, :]
    pen = jnp.where(column < own_count[:, None], 0.0, PENALTY).astype(F32)
    pairs = pair_slots[0, 0]
    delta = lax.rem(pairs // 2 - w + words, words)
    place = jnp.where(delta < reach, 2 * delta, 2 * (words - delta) - 1)
    pairs = place * 2 + lax.rem(pairs, 2)
    live = jnp.where(column < own_count[pairs[:, 0]][:, None], 1.0, 0.0).astype(F32)
    flat_pairs = pairs.reshape(-1)
    sign = 1 - 2 * core
    ahead = lax.rem(w + sign * jnp.arange(1, 5, dtype=I32) + words, words)
    behind = lax.rem(w - sign * (reach - 4) + words, words)
    trims = lax.dynamic_index_in_dim(send_table, behind, 0, keepdims=False).reshape(words, targets)[ahead]
    trims = jnp.concatenate((trims[:3].reshape(-1), lax.dynamic_slice_in_dim(trims[3], core * subs, subs, 0)))

    at_own = (w * subs + s) * per
    listed = jnp.transpose(lax.dynamic_slice_in_dim(neighbours, at_own, per, 1), (1, 0))
    listed = jnp.pad(listed, ((0, 0), (0, padded - topk)))
    itself = at_own + jnp.arange(per, dtype=I32)[:, None] + jnp.zeros((1, padded), I32)

    def locate(image):
        flat = jnp.pad(image.reshape(-1), (0, 4 * LANES - per * padded)).reshape(4, LANES)
        return flat // LANES, lax.rem(flat, LANES)

    near_row, near_lane = locate(listed)
    own_row, own_lane = locate(itself)

    norm_struct = struct((share, LANES), F32)
    first = (partner, norm, cross(1))
    b = send(call(first_kernel, struct((held + 2, depth, points)), first))
    norm = jnp.where(core == 0, norm, 0.0)
    full = reach - 4
    cut = GROUPS[0]
    blocks = [(descriptors,), (a, b)]
    group = None
    exchange = []
    plan = [(0, 1, 2 * cut, 2, 0), (0, 0, 1, 0, 4 * cut), (1, 2 * cut + 1, 2 * (full - cut), 2, 0)]

    def step(k):
        nonlocal group
        d = k - 2
        if d > full:
            return cross(k)
        if d == 0:
            where, tiles = 4 * cut, 4 * cut + 2
        elif d <= cut:
            where, tiles = 4 * (d - 1), 4 * cut + 2
        else:
            where, tiles = 4 * (d - 1 - cut), 4 * (full - cut)
        product, group = cross(k, d, blocks[d], group, where, tiles)
        if d in (cut, full):
            exchange.append(lax.all_to_all(group, "sub", 0, 0, tiled=True))
            group = None
        return product

    for k in range(2, full + 1):
        product = step(k)
        a = send(a)
        merged, norm = call(
            functools.partial(merge_kernel, 0), (struct((held + 2, depth, points)), norm_struct), (b, norm, product)
        )
        b = send(merged)
        blocks.append((a, b))
    size = 3 * targets + subs
    a, b, norm = call(
        trim_kernel,
        (struct((size, depth, points)), struct((size + 2, depth, points)), norm_struct),
        (trims, a, b, norm, step(full + 1)),
        [sm()] + [vm()] * 4,
    )
    a, b = send(a), send(b)
    last = [a, b]
    for k in range(full + 2, reach + 1):
        size -= targets
        product = step(k)
        if k == reach:
            kept = call(keep_kernel, struct((2, 4, LANES), F32), (b, product))
        a = send(a[targets:])
        merged, norm = call(
            functools.partial(merge_kernel, targets),
            (struct((size + 2, depth, points)), norm_struct),
            (b, norm, product),
        )
        b = send(merged)
        last += [a, b]
    steps = len(last) // 2
    tail = call(
        functools.partial(tail_kernel, subs),
        struct((subs, 4 * steps + 2, depth, points)),
        (info, *last, norm, kept),
        [sm()] + [vm()] * (len(last) + 2),
    )
    tail = lax.all_to_all(tail, "sub", 0, 0, tiled=True)

    total = 2 * words
    held_struct = (
        struct((total, points, width + depth)),
        struct((total, width + depth, points)),
        struct((total, points), F32),
    )
    ready = call(
        functools.partial(early_kernel, len(exchange), plan),
        held_struct,
        (info, *exchange, pen),
        [sm()] + [vm()] * (len(exchange) + 1),
    )
    plan = [(0, 2 * full + 1, 2 * (steps - 1), 2, 0), (0, 2 * reach - 1, 1, 1, 4 * (steps - 1))]
    ins = (flat_pairs, info, tail, pen, live, near_row, near_lane, own_row, own_lane, *ready)
    rows = struct((pair_total, points), F32)
    nearest, margin, similarity, *_ = call(
        functools.partial(match_kernel, plan, width, topk, padded),
        (rows, rows, struct((per, topk), F32), *held_struct),
        ins,
        [sm(), sm()] + [vm()] * (len(ins) - 2),
        (
            pltpu.VMEM((pair_total, 8, points), F32),
            pltpu.VMEM((pair_total, 8, points), F32),
            pltpu.VMEM((pair_total, points), F32),
        ),
        4,
        {9: 3, 10: 4, 11: 5},
    )
    return similarity, nearest[None, None], margin[None, None]


def solution(mesh):
    in_specs = (
        P("word", None, "groups"),
        P("word", None, "groups"),
        P(None, "groups"),
        P(("groups", "word"), "sub", None),
        P("groups"),
        P("groups", None, None, None),
        P(("groups", "word"), "sub", None, None),
    )
    out_specs = (
        P(("groups", "word", "sub"), None),
        P(("groups", "word"), "sub", None, None),
        P(("groups", "word"), "sub", None, None),
    )

    return jax.shard_map(local, mesh=mesh, in_specs=in_specs, out_specs=out_specs, check_vma=False)
```

```python
import functools

import jax
import jax.numpy as jnp
from jax import lax
from jax.experimental import pallas as pl
from jax.experimental.pallas import tpu as pltpu
from jax.sharding import PartitionSpec as P


INTERPRET = False
F32, BF16, I32 = jnp.float32, jnp.bfloat16, jnp.int32
LANES = 128
PENALTY = 1e30
SMEM = pltpu.SMEM
VMEM = pltpu.VMEM


def call(body, outs, ins, specs=None, scratch=(), mebibytes=2, aliases=None, outside=(), plain=()):
    specs = specs or [vm() for _ in ins]
    single = not isinstance(outs, (list, tuple))
    out_list = [outs] if single else list(outs)
    ins = [
        pltpu.with_memory_space_constraint(x, VMEM) if spec.memory_space is VMEM and not INTERPRET else x
        for x, spec in zip(ins, specs)
    ]
    gridded = any(spec.block_shape is not None for spec in specs)
    result = pl.pallas_call(
        body,
        out_shape=[x if INTERPRET or i in outside or i in plain else VMEM(x.shape, x.dtype) for i, x in enumerate(out_list)],
        in_specs=specs,
        out_specs=[pl.BlockSpec(memory_space=pl.ANY) if i in outside else vm() for i in range(len(out_list))],
        **({"grid": (1,)} if gridded else {}),
        scratch_shapes=list(scratch),
        input_output_aliases=aliases or {},
        compiler_params=pltpu.CompilerParams(vmem_limit_bytes=mebibytes << 20),
        interpret=INTERPRET,
    )(*ins)
    return result[0] if single else result


def vm():
    return pl.BlockSpec(memory_space=VMEM)


def sm():
    return pl.BlockSpec(memory_space=SMEM)


def outside_vmem(arrays):
    return arrays if INTERPRET else [pltpu.with_memory_space_constraint(x, pltpu.HBM) for x in arrays]


def struct(shape, dtype=BF16):
    return jax.ShapeDtypeStruct(shape, dtype)


def rounded(x):
    return x.astype(BF16).astype(F32)


def split3(x):
    first = rounded(x)
    rest = x - first
    second = rounded(rest)
    return first, second, rounded(rest - second)


def encode(norms, dots):
    high = rounded(norms)
    low = rounded(norms - high)
    return jnp.concatenate((high, low) + split3(dots), axis=0).astype(BF16)


def decode(tile):
    wide = tile.astype(F32)
    norms = wide[0:2] + wide[2:4]
    dots = (wide[4:8] + wide[8:12]) + wide[12:16]
    return norms, dots, wide[0:4]


def re_encode(head, dots):
    return jnp.concatenate((head,) + split3(dots), axis=0).astype(BF16)


def spread(rows):
    turned = pltpu.roll(rows, 64, 1)
    low = lax.broadcasted_iota(I32, rows.shape, 1) < 64
    return jnp.where(low, rows, turned), jnp.where(low, turned, rows)


def staggered(four):
    group = lax.broadcasted_iota(I32, four.shape, 1) // 32
    out = four
    for g in range(1, 4):
        out = jnp.where(group == g, pltpu.roll(four, LANES - 8 * g, 1), out)
    return out


def lane_sums(products):
    ones = jnp.ones((8, LANES), BF16)
    total = None
    for term in split3(products):
        part = lax.dot_general(ones, term.astype(BF16), (((1,), (1,)), ((), ())), preferred_element_type=F32)
        total = part if total is None else total + part
    return total


def table_kernel(info, ids_ref, values_ref, table_ref, norm_ref):
    occurrences, images = ids_ref.shape
    for j in range(images // LANES):
        lanes = slice(j * LANES, (j + 1) * LANES)
        ids, values = ids_ref[:, lanes].astype(F32), values_ref[:, lanes]
        table_ref[lanes, :] = jnp.concatenate((ids, ids, values, values), axis=0).T
    share = norm_ref.shape[0]
    for j in range(share):
        start = pl.multiple_of((info[1] * share + j) * LANES, LANES)
        ids, values = ids_ref[:, pl.ds(start, LANES)], values_ref[:, pl.ds(start, LANES)]
        acc = jnp.zeros_like(values)
        for b in range(occurrences):
            acc = acc + jnp.where(ids == ids[b : b + 1], values[b : b + 1], 0.0)
        norm_ref[j : j + 1, :] = jnp.sum(acc * values, axis=0, keepdims=True)


def pick_images(distance, step, info, taken, blocks, group_ref, picked, stored):
    core = info[0]
    paired = len(blocks) - 1
    for s in range(picked.shape[0]):
        for c in range(2):
            slot = taken[distance * 2 * picked.shape[0] + 2 * s + c]
            if paired:
                picked[s, 2 * c + core] = blocks[0][slot]
                picked[s, 2 * c + 1 - core] = blocks[1][slot]
            else:
                picked[s, c] = blocks[0][slot]
    tiles = 2 + 2 * paired
    store = pltpu.make_async_copy(picked.at[:, 0:tiles], group_ref.at[:, step : step + tiles], stored)
    store.start()
    return store


def pick_kernel(distance, step, info, taken, block_a, block_b, group_in, group_ref, picked, stored):
    del group_in
    pick_images(distance, step, info, taken, (block_a, block_b), group_ref, picked, stored).wait()


def cross_kernel(count, k, turn, words, chosen, deps, info, lists, table_ref, rows_ref, *refs):
    idx, arrived, picked, stored = refs[-4:]
    refs = refs[deps:-4]
    fetch = pltpu.make_async_copy(lists.at[k - 1], idx, arrived)
    fetch.start()
    if chosen is None:
        out_ref, turned, gathered, products = refs
    else:
        distance, step, paired, fresh = chosen
        taken, refs = refs[0], refs[1:]
        blocks, refs = refs[: 1 + paired], refs[1 + paired + (not fresh) :]
        out_ref, group_ref, turned, gathered, products = refs
        store = pick_images(distance, step, info, taken, blocks, group_ref, picked, stored)
    padded = gathered.shape[1]
    total = turned.shape[2]
    half = total // 2
    up, down = turn
    target = lax.rem(info[3] + jnp.where(info[0] == 0, up, down), words)
    start = pl.multiple_of((target * (rows_ref.shape[0] // (words * total)) + info[1]) * total, total)
    ids, weights = spread(rows_ref[pl.ds(start, total), :])
    other, value = staggered(ids), staggered(weights)
    for t in range(8):
        turned[0, t] = pltpu.roll(other, LANES - t, 1) if t else other
        turned[1, t] = pltpu.roll(value, LANES - t, 1) if t else value
    empty = jnp.zeros((8, LANES), F32)
    for e in range(2):
        gathered[e, padded - 8 :, :] = empty
        for part in range(half * padded // 8, 4 * LANES // 8):
            products[e, part * 8 : part * 8 + 8, :] = empty

    fetch.wait()

    def image(i, carry):
        for e in range(2):
            for k in range(count):
                row = idx[0, (e * half + i) * count + k]
                gathered[e, k : k + 1, :] = table_ref[row]
        for e in range(2):
            queries = [turned[0, t, pl.ds(e * half + i, 1), :] for t in range(8)]
            scales = [turned[1, t, pl.ds(e * half + i, 1), :] for t in range(8)]
            for part in range(padded // 8):
                near_ids, near_weights = spread(gathered[e, part * 8 : part * 8 + 8, :])
                acc = jnp.zeros_like(near_ids)
                for t in range(8):
                    acc = acc + jnp.where(near_ids == queries[t], scales[t], 0.0)
                at = pl.multiple_of(i * padded + part * 8, 8)
                products[e, pl.ds(at, 8), :] = acc * near_weights
        return carry

    lax.fori_loop(0, half, image, 0)
    for e in range(2):
        sums = lane_sums(products[e])
        for j in range(4):
            out_ref[e, j : j + 1, :] = sums[0:1, j * LANES : (j + 1) * LANES]
    if chosen is not None:
        store.wait()


def first_kernel(desc_ref, norm_ref, cross_ref, out):
    held = desc_ref.shape[0]
    out[0:held] = desc_ref[...]
    for e in range(2):
        out[held + e] = encode(norm_ref[2 * e : 2 * e + 2], cross_ref[e])


def merge_kernel(skip, recv, norm_ref, cross_ref, out, norm_out):
    kept = out.shape[0] - 2
    last = recv.shape[0] - 2
    out[0:kept] = recv[skip : skip + kept]
    for e in range(2):
        norms, dots, head = decode(recv[last + e])
        out[kept + e] = re_encode(head, dots + cross_ref[e])
        norm_out[2 * e : 2 * e + 2] = norm_ref[2 * e : 2 * e + 2] + norms


def trim_kernel(idx, recv_a, recv_b, norm_ref, cross_ref, out_a, out_b, norm_out):
    kept = out_a.shape[0]
    last = recv_b.shape[0] - 2
    for n in range(kept):
        out_a[n] = recv_a[idx[n]]
        out_b[n] = recv_b[idx[n]]
    for e in range(2):
        norms, dots, head = decode(recv_b[last + e])
        out_b[kept + e] = re_encode(head, dots + cross_ref[e])
        norm_out[2 * e : 2 * e + 2] = norm_ref[2 * e : 2 * e + 2] + norms


def tail_kernel(subs, info, *refs):
    blocks, (norm_ref, kept_ref, out) = refs[:-3], refs[-3:]
    core = info[0]
    last = len(blocks) // 2 - 1
    for j in range(last + 1):
        for q, src in ((core, blocks[2 * j]), (1 - core, blocks[2 * j + 1])):
            for s in range(subs):
                for c in range(2):
                    slot = 2 * s + c if j < last else 2 * (s % (subs // 2)) + c
                    out[s, 4 * j + 2 * c + q] = src[slot]
    recv = blocks[-1]
    size = recv.shape[0] - 2
    upward = core == 0
    totals = []
    empty = jnp.zeros((4, LANES), F32)
    for e in range(2):
        norms, dots, _ = decode(recv[size + e])
        totals.append(norm_ref[2 * e : 2 * e + 2] + jnp.where(upward, norms, 0.0))
        own = jnp.where(upward, dots, kept_ref[e])
        tile = jnp.concatenate(split3(own) + (empty,), axis=0).astype(BF16)
        for s in range(subs // 2):
            out[2 * s + e, 4 * last + 5] = tile
    tile = jnp.concatenate(split3(jnp.concatenate(totals, axis=0)) + (empty,), axis=0).astype(BF16)
    for s in range(subs):
        out[s, 4 * last + 4] = tile


def keep_kernel(recv, cross_ref, out):
    last = recv.shape[0] - 2
    for e in range(2):
        _, dots, _ = decode(recv[last + e])
        out[e] = dots + cross_ref[e]


def joined(tile):
    wide = tile.astype(F32)
    return (wide[0:4] + wide[4:8]) + wide[8:12]


def operands(plan, info, groups, pen, lhs, rhs, squares):
    subs = groups[0].shape[0]
    depth = groups[0].shape[2]
    row = lax.broadcasted_iota(I32, (depth, LANES), 0)
    ones = jnp.where(row < 4, 1.0, 0.0).astype(BF16)

    def prepare(slot, blocks):
        total = jnp.zeros((depth, LANES), F32)
        scaled = []
        for s, block in enumerate(blocks):
            rhs[slot, s * depth : (s + 1) * depth, :] = block
            value = block.astype(F32)
            scaled.append(value * -2.0)
            total = total + value * value
        square = jnp.sum(total, axis=0, keepdims=True)
        squares[pl.ds(slot, 1), :] = square
        parts = split3(square)
        extra = jnp.where(row == 0, parts[0], 0.0)
        extra = jnp.where(row == 1, parts[1], extra)
        extra = jnp.where(row == 2, parts[2], extra)
        scaled.append(jnp.where(row == 3, pen[pl.ds(slot, 1), :], extra))
        rhs[slot, subs * depth :, :] = ones
        lhs[slot] = jnp.concatenate(scaled, axis=0).T.astype(BF16)

    for which, first, positions, ways, at in plan:
        group = groups[which]

        def image(i, carry, group=group, first=first, ways=ways, at=at):
            if ways == 0:
                prepare(i, [group[s, at + i] for s in range(subs)])
                return carry
            source = i // 2
            step = source // ways
            lineage = source - ways * step if ways == 2 else info[2]
            tile = at + 4 * step + 2 * (i - 2 * source)
            prepare(2 * first + i, [group[2 * (s // 2) + lineage, tile + s % 2] for s in range(subs)])
            return carry

        lax.fori_loop(0, 2 * positions, image, 0)


def early_kernel(count, plan, info, *refs):
    pen, lhs, rhs, squares = refs[count:]
    operands(plan, info, refs[:count], pen, lhs, rhs, squares)


def joined(tile):
    wide = tile.astype(F32)
    return (wide[0:4] + wide[4:8]) + wide[8:12]


def match_kernel(plan, width, topk, padded, pairs, info, *refs):
    group, pen, live, near_row, near_lane, own_row, own_lane, lhs_in, rhs_in, squares_in = refs[:10]
    nearest, margin, similarity, lhs, rhs, squares, least, less, query, left, right = refs[10:]
    ready = lhs_in.shape[0]
    bring = (
        pltpu.make_async_copy(lhs_in, lhs.at[0:ready], left),
        pltpu.make_async_copy(rhs_in, rhs.at[0:ready], right),
    )
    for copy in bring:
        copy.start()
    squares[0:ready] = squares_in[...]
    pair_total = nearest.shape[0]
    subs = group.shape[0]
    end = group.shape[1]
    operands(plan, info, [group], pen, lhs, rhs, squares)

    near = jnp.zeros(near_row.shape, F32)
    own = jnp.zeros(near_row.shape, F32)
    for x in range(subs // 2):
        rows = joined(group[2 * x, end - 2]) + joined(group[2 * x + 1, end - 2])
        for h in range(4):
            line = jnp.broadcast_to(rows[h : h + 1], near_row.shape)
            at = jnp.take_along_axis(line, near_lane[...], axis=1)
            near = jnp.where(near_row[...] == 4 * x + h, at, near)
            at = jnp.take_along_axis(line, own_lane[...], axis=1)
            own = jnp.where(own_row[...] == 4 * x + h, at, own)
    chip = info[1]
    dots = joined(group[2 * chip, end - 1]) + joined(group[2 * chip + 1, end - 1])
    cosine = dots / jnp.sqrt(own * near)
    for r in range(similarity.shape[0]):
        line, lane = divmod(r * padded, LANES)
        both = jnp.concatenate((cosine[line : line + 1], cosine[line + 1 : line + 2]), axis=1) if line < 3 else cosine[3:4]
        similarity[r : r + 1, :] = both[:, lane : lane + topk]

    for copy in bring:
        copy.wait()

    def pair(p, carry):
        asked = pairs[2 * p]
        refer = pairs[2 * p + 1]
        scores = jnp.dot(lhs[refer], rhs[asked], preferred_element_type=F32)
        first = scores[0:8]
        second = jnp.full_like(first, PENALTY)
        for b in range(1, LANES // 8):
            value = scores[8 * b : 8 * b + 8]
            second = jnp.minimum(second, jnp.maximum(first, value))
            first = jnp.minimum(first, value)
        least[p] = first
        less[p] = second
        query[pl.ds(p, 1), :] = squares[pl.ds(asked, 1), :]
        return carry

    def four(q, carry):
        for r in range(4):
            pair(4 * q + r, carry)
        return carry

    if pair_total % 4 == 0:
        lax.fori_loop(0, pair_total // 4, four, 0)
    else:
        lax.fori_loop(0, pair_total, pair, 0)
    first = least[:, 0, :]
    second = less[:, 0, :]
    for b in range(1, 8):
        other, runner = least[:, b, :], less[:, b, :]
        second = jnp.minimum(jnp.maximum(first, other), jnp.minimum(second, runner))
        first = jnp.minimum(first, other)
    alive = live[...] > 0.0
    nearest[...] = jnp.where(alive, (first + query[...]) * (1.0 / width), 0.0)
    margin[...] = jnp.where(alive, (second - first) * (1.0 / width), 0.0)


def local(word_ids, word_weights, neighbours, descriptors, keypoint_count, send_table, pair_slots):
    words = lax.axis_size("word")
    subs = lax.axis_size("sub")
    w = lax.axis_index("word")
    s = lax.axis_index("sub")
    core = lax.rem(s, 2)
    reach = words // 2
    pairs_of_ring = [
        (i * subs + j, ((i + (1 if j % 2 == 0 else words - 1)) % words) * subs + j)
        for i in range(words)
        for j in range(subs)
    ]
    _, images = word_ids.shape[1:]
    topk = neighbours.shape[0]
    padded = -(-topk // 8) * 8
    per = images // (words * subs)
    held, depth, points = descriptors.shape
    targets = 2 * subs
    width = depth * subs
    pair_total = pair_slots.shape[2]

    def send(x):
        return lax.ppermute(x, ("word", "sub"), pairs_of_ring)

    a = send(descriptors)
    partner = lax.ppermute(descriptors, "sub", [(j, j ^ 1) for j in range(subs)])

    chips = subs // 2
    chip = s // 2
    info = jnp.stack((core, chip, s // chips, w)).astype(I32)
    share = images // chips // LANES
    table, norm = call(
        table_kernel,
        (struct((images, LANES), F32), struct((share, LANES), F32)),
        (info, word_ids[0], word_weights[0]),
        [sm(), vm(), vm()],
        (),
        4,
    )
    table3 = table.reshape(images, 1, LANES)
    near = lax.dynamic_index_in_dim(neighbours.reshape(topk, words, chips, 2 * per), chip, 2, keepdims=False)
    near = jnp.transpose(near, (1, 2, 0)).reshape(words, 2 * per * topk)
    count = jnp.arange(1, reach + 1, dtype=I32)
    turn = lax.rem(w + jnp.where(core == 0, reach + 1 - count, reach + count), words)
    near_order = near[turn].reshape(reach, 1, 2 * per * topk)
    away = jnp.arange(0, reach, dtype=I32)
    taken_here = lax.dynamic_index_in_dim(send_table, w, 1, keepdims=False).reshape(words, targets)
    taken_mine = taken_here[lax.rem(w + jnp.where(core == 0, words - away, away), words)].reshape(-1)

    def cross(k, deps=(), distance=None, sources=(), group=None, step=0, tiles=0):
        apart = pl.BlockSpec(memory_space=pl.ANY)
        specs = [sm(), apart, vm(), vm()] + [apart] * len(deps)
        ins = [info, near_order, table3, table, *deps]
        outs = [struct((2, 4, LANES), F32)]
        chosen, aliases = None, {}
        if sources:
            chosen = (distance, step, len(sources) - 1, group is None)
            specs += [sm()]
            ins += [taken_mine, *sources]
            specs += [vm()] * len(sources)
            outs += [struct((subs, tiles, depth, points))]
            if group is not None:
                aliases = {len(ins): 1}
                ins += [group]
                specs += [apart]
        result = call(
            functools.partial(cross_kernel, topk, k, (reach + 1 - k, reach + k), words, chosen, len(deps)),
            outs,
            ins,
            specs,
            (
                pltpu.VMEM((2, 8, 2 * per, LANES), F32),
                pltpu.VMEM((2, padded, LANES), F32),
                pltpu.VMEM((2, 4 * LANES, LANES), F32),
                pltpu.SMEM((1, 2 * per * topk), I32),
                pltpu.SemaphoreType.DMA(()),
                pltpu.VMEM((subs, 4, depth, points), BF16),
                pltpu.SemaphoreType.DMA(()),
            ),
            4,
            aliases,
            {1},
        )
        return result if sources else result[0]

    order = [0]
    for d in range(1, reach):
        order += [words - d, d]
    order += [reach]
    source = lax.rem(w + jnp.array(order, I32), words)
    taken = taken_here[source]
    own_images = lax.dynamic_slice_in_dim(taken, 2 * s, 2, 1) + source[:, None] * held
    own_count = keypoint_count[own_images.reshape(-1)]
    column = jnp.arange(points, dtype=I32)[None, :]
    pen = jnp.where(column < own_count[:, None], 0.0, PENALTY).astype(F32)
    pairs = pair_slots[0, 0]
    delta = lax.rem(pairs // 2 - w + words, words)
    place = jnp.where(delta < reach, 2 * delta, 2 * (words - delta) - 1)
    pairs = place * 2 + lax.rem(pairs, 2)
    live = jnp.where(column < own_count[pairs[:, 0]][:, None], 1.0, 0.0).astype(F32)
    flat_pairs = pairs.reshape(-1)
    sign = 1 - 2 * core
    ahead = lax.rem(w + sign * jnp.arange(1, 5, dtype=I32) + words, words)
    behind = lax.rem(w - sign * (reach - 4) + words, words)
    trims = lax.dynamic_index_in_dim(send_table, behind, 0, keepdims=False).reshape(words, targets)[ahead]
    trims = jnp.concatenate((trims[:3].reshape(-1), lax.dynamic_slice_in_dim(trims[3], core * subs, subs, 0)))

    at_own = (w * subs + s) * per
    listed = jnp.transpose(lax.dynamic_slice_in_dim(neighbours, at_own, per, 1), (1, 0))
    listed = jnp.pad(listed, ((0, 0), (0, padded - topk)))
    itself = at_own + jnp.arange(per, dtype=I32)[:, None] + jnp.zeros((1, padded), I32)

    def locate(image):
        flat = jnp.pad(image.reshape(-1), (0, 4 * LANES - per * padded)).reshape(4, LANES)
        return flat // LANES, lax.rem(flat, LANES)

    near_row, near_lane = locate(listed)
    own_row, own_lane = locate(itself)

    norm_struct = struct((share, LANES), F32)
    first = (partner, norm, cross(1))
    b = send(call(first_kernel, struct((held + 2, depth, points)), first))
    norm = jnp.where(core == 0, norm, 0.0)
    full = reach - 4
    blocks = [(descriptors,), (a, b)]
    group = None
    tiles = 4 * full + 2
    plan = [(0, 1, 2 * full, 2, 0), (0, 0, 1, 0, 4 * full)]
    deps = {4: (trims,), 5: (flat_pairs,), 6: (pen,), 7: (live,), 8: (near_row, near_lane), 9: (own_row, own_lane)}
    late = {k: cross(k) for k in range(full + 1, reach + 1)}

    def step(k):
        nonlocal group
        d = k - 2
        if k <= full:
            where = 4 * (d - 1) if d else 4 * full
            product, group = cross(k, deps.get(k, ()), d, blocks[d], group, where, tiles)
            return product
        if d <= full:
            group = call(
                functools.partial(pick_kernel, d, 4 * (d - 1)),
                struct((subs, tiles, depth, points)),
                (info, taken_mine, *blocks[d], group),
                [sm(), sm(), vm(), vm(), pl.BlockSpec(memory_space=pl.ANY)],
                (pltpu.VMEM((subs, 4, depth, points), BF16), pltpu.SemaphoreType.DMA(())),
                2,
                {4: 0},
                {0},
            )
        return late[k]

    for k in range(2, full + 1):
        product = step(k)
        a = send(a)
        merged, norm = call(
            functools.partial(merge_kernel, 0), (struct((held + 2, depth, points)), norm_struct), (b, norm, product)
        )
        b = send(merged)
        blocks.append((a, b))
    size = 3 * targets + subs
    a, b, norm = call(
        trim_kernel,
        (struct((size, depth, points)), struct((size + 2, depth, points)), norm_struct),
        (trims, a, b, norm, step(full + 1)),
        [sm()] + [vm()] * 4,
    )
    a, b = send(a), send(b)
    last = [a, b]
    for k in range(full + 2, reach + 1):
        size -= targets
        product = step(k)
        if k == full + 2:
            exchange = [lax.all_to_all(group, "sub", 0, 0, tiled=True)]
        if k == reach:
            kept = call(keep_kernel, struct((2, 4, LANES), F32), (b, product))
        a = send(a[targets:])
        merged, norm = call(
            functools.partial(merge_kernel, targets),
            (struct((size + 2, depth, points)), norm_struct),
            (b, norm, product),
        )
        b = send(merged)
        last += [a, b]
    steps = len(last) // 2
    tail = call(
        functools.partial(tail_kernel, subs),
        struct((subs, 4 * steps + 2, depth, points)),
        (info, *last, norm, kept),
        [sm()] + [vm()] * (len(last) + 2),
    )
    tail = lax.all_to_all(tail, "sub", 0, 0, tiled=True)

    total = 2 * words
    early = 2 * (2 * full + 1)
    held_struct = (
        struct((early, points, width + depth)),
        struct((early, width + depth, points)),
        struct((early, points), F32),
    )
    ready = call(
        functools.partial(early_kernel, len(exchange), plan),
        held_struct,
        (info, *exchange, pen),
        [sm()] + [vm()] * (len(exchange) + 1),
        (),
        12,
        None,
        (),
        {0, 1},
    )
    plan = [(0, 2 * full + 1, 2 * (steps - 1), 2, 0), (0, 2 * reach - 1, 1, 1, 4 * (steps - 1))]
    ins = (flat_pairs, info, tail, pen, live, near_row, near_lane, own_row, own_lane, *outside_vmem(ready[:2]), ready[2])
    rows = struct((pair_total, points), F32)
    nearest, margin, similarity = call(
        functools.partial(match_kernel, plan, width, topk, padded),
        (rows, rows, struct((per, topk), F32)),
        ins,
        [sm(), sm()] + [vm()] * (len(ins) - 5) + [pl.BlockSpec(memory_space=pl.ANY)] * 2 + [vm()],
        (
            pltpu.VMEM((total, points, width + depth), BF16),
            pltpu.VMEM((total, width + depth, points), BF16),
            pltpu.VMEM((total, points), F32),
            pltpu.VMEM((pair_total, 8, points), F32),
            pltpu.VMEM((pair_total, 8, points), F32),
            pltpu.VMEM((pair_total, points), F32),
            pltpu.SemaphoreType.DMA(()),
            pltpu.SemaphoreType.DMA(()),
        ),
        10,
    )
    return similarity, nearest[None, None], margin[None, None]


def solution(mesh):
    in_specs = (
        P("word", None, "groups"),
        P("word", None, "groups"),
        P(None, "groups"),
        P(("groups", "word"), "sub", None),
        P("groups"),
        P("groups", None, None, None),
        P(("groups", "word"), "sub", None, None),
    )
    out_specs = (
        P(("groups", "word", "sub"), None),
        P(("groups", "word"), "sub", None, None),
        P(("groups", "word"), "sub", None, None),
    )

    return jax.shard_map(local, mesh=mesh, in_specs=in_specs, out_specs=out_specs, check_vma=False)
```
